128 devices in a mesh: expert: 8 (over z, x_hi), dp: 16 (over x_lo, y, core).
Axes of the slice: x: 4 (x_hi: 2, x_lo: 2; x = x_hi * 2 + x_lo), y: 4, z: 4, core: 2. Of those that a mesh axis runs over, the one named last changes fastest.
Arguments:
- tokens: bfloat16 [16384, 3584], P(('expert', 'dp')), may hold values from -24 to 24
- cotangent: bfloat16 [16384, 3584], P(('expert', 'dp')), may hold values from -1.5 to 1.5
- block_expert: int32 [1024, 1], P(('expert', 'dp')), may hold values from 0 to 7; in each aligned block of 8 rows (0 to 7, 8 to 15, ...) at most 2 rows name the same one
- block_count: int32 [1024], P(('expert', 'dp')), may hold values from 8 to 16
- old_owner: int32 [8], replicated, may hold values from 0 to 7, as said below
- new_owner: int32 [8], replicated, may hold values from 0 to 7, as said below
- up_weight: float32 [8, 3584, 1024], P('expert', 'dp'), may hold values from -0.09375 to 0.09375
- down_weight: float32 [8, 1024, 3584], P('expert', 'dp'), may hold values from -0.1875 to 0.1875
- up_first: float32 [8, 3584, 1024], P('expert', 'dp'), may hold values from -6 to 6
- up_second: float32 [8, 3584, 1024], P('expert', 'dp'), may hold values from 1 to 100
- down_first: float32 [8, 1024, 3584], P('expert', 'dp'), may hold values from -6 to 6
- down_second: float32 [8, 1024, 3584], P('expert', 'dp'), may hold values from 1 to 100
Outputs:
- token_grad: bfloat16 [16384, 3584], P(('expert', 'dp'))
- up_weight_new: float32 [8, 3584, 1024], P('expert', 'dp')
- down_weight_new: float32 [8, 1024, 3584], P('expert', 'dp')
- up_first_new: float32 [8, 3584, 1024], P('expert', 'dp')
- up_second_new: float32 [8, 3584, 1024], P('expert', 'dp')
- down_first_new: float32 [8, 1024, 3584], P('expert', 'dp')
- down_second_new: float32 [8, 1024, 3584], P('expert', 'dp')
The draws below stay inside these ranges and needn't reach their ends.
Inputs may be any that keep to these rules, and one draw needn't show every extreme that they name: `block_expert`: among the 8 blocks of one device, at most 2 are routed to any one expert, and in every draw some device routes exactly 2 blocks to some expert. A permutation: each slot appears once, and expert k is held by slot old_owner[k] before the step. A permutation: each slot appears once, and expert k is held by slot new_owner[k] after the step.
All inputs are finite; a program needn't handle non-finite values.
Results may differ from the reference program's by a relative error of at most 0.019.
Values may be sent and summed in bfloat16 or wider, within the bound.
No kernel may reach another device: no remote copies, remote signals or barrier semaphores. Data moves between devices by JAX's collectives and lax.ppermute only.
A program may use at most 192 MiB of HBM per device.

```python
import math
import jax
import jax.numpy as jnp
import numpy as np
from jax import lax

D = 3584
FF = 1024
BLOCK_TOK = 16
BLOCKS_DEV = 8
CAPACITY = 2
EXPERTS = 8
TOKENS = 16384
BLOCKS = 1024
N_EXPERT = 8
N_DP = 16


def ranked_order(key, salt):
    inner = jax.random.fold_in(key, salt)
    scores = jax.random.randint(inner, (EXPERTS,), 0, 1 << 20, dtype=jnp.int32)
    distinct = scores * EXPERTS + jnp.arange(EXPERTS, dtype=jnp.int32)
    return jnp.argsort(distinct, stable=True).astype(jnp.int32)


def draw_old_owner(key, part):
    return ranked_order(key, 7101)


def draw_new_owner(key, part):
    return ranked_order(key, 9203)


def place_ends(drawn, own_key, smallest, top_value):
    longest = drawn.shape.index(max(drawn.shape))
    spots = []
    for shift in (0, 1):
        where = [jax.random.randint(jax.random.fold_in(own_key, axis), (), 0, length) for axis, length in enumerate(drawn.shape)]
        where[longest] = (where[longest] + shift) % drawn.shape[longest]
        spots.append(tuple(where))
    return drawn.at[spots[0]].set(smallest).at[spots[1]].set(top_value)


def with_spikes(drawn, stream_key, source, target, blocks, factor):
    owner, partner = [(jnp.arange(drawn.shape[axis_at]) // (drawn.shape[axis_at] // blocks)).reshape([-1 if axis == axis_at else 1 for axis in range(drawn.ndim)]) for axis_at in (source, target)]
    chosen = jax.random.permutation(stream_key, blocks)[partner]
    strong = (owner == chosen) | (owner == (partner + blocks // 2) % blocks)
    return jnp.where(strong, factor * drawn, drawn)


def block_scale(stream_key, extent, pieces, least, high):
    def one(dim, shards_of):
        heights = jax.random.uniform(jax.random.fold_in(jax.random.fold_in(stream_key, 6), dim), (shards_of,), jnp.float32, least / len(pieces), high / len(pieces))
        return jnp.repeat(jnp.exp(heights), extent[dim] // shards_of).reshape((-1,) + (1,) * (len(extent) - dim - 1))

    gain = one(*pieces[0])
    for cut in pieces[1:]:
        gain = gain * one(*cut)
    return gain


def assign_block(rng, own, number, rows, count, top, bound, slope):
    ranking = jax.random.permutation(rng, count)
    heavy_load, common = portions_of(count, rows * top, bound, slope, True), portions_of(count, rows * top, bound, slope, False)
    places = jnp.arange(count)

    def named(lengths, offset_by):
        used = int((lengths > 0).sum())
        fixed = max(1, used // 4)
        passed = fixed + (places - fixed + offset_by * (used - fixed)) % max(1, count - fixed)
        return jnp.zeros((count,), jnp.int32).at[ranking[jnp.where(places < fixed, places, passed)]].set(jnp.asarray(lengths, jnp.int32))

    lengths = jnp.where(number % 4 == 0, named(heavy_load, number // 4), named(common, number - number // 4 - 1))
    mixed = jax.random.permutation(jax.random.fold_in(own, 3), count)
    donor, taker = mixed[0:count // 2 * 2:2], mixed[1:count // 2 * 2:2]
    room = jnp.minimum(lengths[donor] - 1, bound - lengths[taker]) // 2
    room = jnp.where((donor == ranking[0]) | (taker == ranking[0]) | (lengths[taker] == 0), 0, jnp.maximum(room, 0))
    passed = jax.random.randint(jax.random.fold_in(own, 4), (count // 2,), 0, 1 << 20) % (room + 1)
    lengths = lengths.at[donor].add(-passed).at[taker].add(passed)
    items = jnp.searchsorted(jnp.cumsum(lengths), jnp.arange(rows * top), side="right").astype(jnp.int32)
    table = items.reshape(top, rows).T
    table = table[jax.random.permutation(jax.random.fold_in(own, 1), rows)]
    offset_by = jax.random.randint(jax.random.fold_in(own, 2), (rows, 1), 0, top)
    return jnp.take_along_axis(table, (jnp.arange(top)[None, :] + offset_by) % top, axis=1)


def portions_of(count, total, most, skew, full):
    loads = [(1 << 20) // math.isqrt(rank ** skew) + 1 for rank in range(1, count + 1)]
    largest = most if full else min(most, max(-(-total // count), total * loads[0] // sum(loads)))
    least = 1 if total - largest >= count - 1 else 0
    given, surplus = [largest] + [least] * (count - 1), total - largest - least * (count - 1)
    while surplus > 0:
        candidates = [i for i in range(1, count) if given[i] < largest] or [i for i in range(1, count) if given[i] < most]
        mass, remaining = sum([loads[i] for i in candidates]), surplus
        for i in candidates:
            extra = min(most - given[i], max(1, remaining * loads[i] // mass), surplus)
            given[i] = given[i] + extra
            surplus = surplus - extra
    return np.array(given)


def bell_draw(key, extent, spread, most, cuts=(), held_as=jnp.bfloat16):
    gain = block_scale(key, extent, cuts, -0.22, 0.18) if cuts else 1.0
    result = jax.random.normal(key, extent, jnp.float32) * spread * gain
    return jnp.minimum(jnp.maximum(result, -most), most).astype(held_as)


def heavy_noise(own_key, shape, deviation, reach, pieces, heavy, kind=jnp.bfloat16):
    array = deviation * jax.random.normal(own_key, shape, jnp.float32)
    if pieces:
        array = array * block_scale(own_key, shape, pieces, -0.22, 0.18)
    return jnp.clip(with_spikes(array, jax.random.fold_in(own_key, 3), *heavy), -reach, reach).astype(kind)


def setup_inputs(seed: int = 0) -> dict:
    splits = jax.random.split(jax.random.key(seed), 13)
    tokens = heavy_noise(splits[0], (TOKENS, D), 1.0, 24.0, ((0, 128),), (0, 1, 128, 5.5))
    cotangent = bell_draw(splits[1], (TOKENS, D), 0.25, 1.5, ((0, 128),))
    block_expert_keys = jax.random.split(jax.random.fold_in(splits[2], 1), BLOCKS // BLOCKS_DEV)
    block_expert_turns = jax.random.permutation(jax.random.fold_in(splits[2], 3), BLOCKS // BLOCKS_DEV)
    block_expert = jax.vmap(lambda own, number: assign_block(jax.random.fold_in(splits[2], 2), own, number, BLOCKS_DEV, EXPERTS, 1, CAPACITY, 2))(block_expert_keys, block_expert_turns).reshape((BLOCKS, 1))
    block_count = place_ends(jax.random.randint(splits[3], (BLOCKS,), BLOCK_TOK // 2, BLOCK_TOK + 1), jax.random.fold_in(splits[3], 1), BLOCK_TOK // 2, BLOCK_TOK).astype(jnp.int32)
    old_owner = draw_old_owner(jax.random.fold_in(splits[12], 71), 0)
    new_owner = draw_new_owner(jax.random.fold_in(splits[12], 71), 0)
    up_weight = bell_draw(splits[6], (EXPERTS, D, FF), D ** -0.5, 0.09375, ((0, 8), (1, 16)), jnp.float32)
    down_weight = bell_draw(splits[7], (EXPERTS, FF, D), FF ** -0.5, 0.1875, ((0, 8), (1, 16)), jnp.float32)
    up_first = bell_draw(splits[8], (EXPERTS, D, FF), 1.0, 6.0, ((0, 8), (1, 16)), jnp.float32)
    up_second = jnp.clip(jnp.exp(math.log(100.0) - 4.6051702 * jax.random.uniform(splits[9], (EXPERTS, D, FF), jnp.float32) ** block_scale(splits[9], (EXPERTS, D, FF), ((0, 8), (1, 16)), -0.2, 0.2)), 1.0, 100.0)
    down_first = bell_draw(splits[10], (EXPERTS, FF, D), 1.0, 6.0, ((0, 8), (1, 16)), jnp.float32)
    down_second = jnp.clip(jnp.exp(math.log(100.0) - 4.6051702 * jax.random.uniform(splits[11], (EXPERTS, FF, D), jnp.float32) ** block_scale(splits[11], (EXPERTS, FF, D), ((0, 8), (1, 16)), -0.2, 0.2)), 1.0, 100.0)
    return dict(tokens=tokens, cotangent=cotangent, block_expert=block_expert, block_count=block_count, old_owner=old_owner, new_owner=new_owner, up_weight=up_weight, down_weight=down_weight, up_first=up_first, up_second=up_second, down_first=down_first, down_second=down_second)


beta_one = 0.9
beta_two = 0.95
bias_one = 1.0 - 0.9 ** 10
bias_two = 1.0 - 0.95 ** 10
rate_value = 0.01
decay_value = 0.1
eps_value = 1e-08

def silu_parts(pre_act):
    sigma = jax.nn.sigmoid(pre_act)
    return (pre_act * sigma, sigma * (1.0 + pre_act * (1.0 - sigma)))

def adam_update(weight, moment, second, gradient):
    moment_new = beta_one * moment + (1.0 - beta_one) * gradient
    second_new = beta_two * second + (1.0 - beta_two) * gradient * gradient
    update = moment_new / bias_one / (jnp.sqrt(second_new / bias_two) + eps_value)
    return (weight - rate_value * (update + decay_value * weight), moment_new, second_new)

def reference(tokens, cotangent, block_expert, block_count, old_owner, new_owner, up_weight, down_weight, up_first, up_second, down_first, down_second):
    groups = N_EXPERT
    ranks = N_DP
    shape = (groups, ranks, BLOCKS_DEV, BLOCK_TOK, D)
    counts = block_count.reshape(groups, ranks, BLOCKS_DEV)
    alive = jnp.arange(BLOCK_TOK, dtype=jnp.int32)[None, None, None, :] < counts[..., None]
    inputs = jnp.where(alive[..., None], tokens.reshape(shape), jnp.zeros((), tokens.dtype))
    upstream = jnp.where(alive[..., None], cotangent.reshape(shape), jnp.zeros((), cotangent.dtype))
    block_ids = block_expert.reshape(groups, ranks, BLOCKS_DEV)
    earlier = jnp.arange(BLOCKS_DEV, dtype=jnp.int32)[:, None] > jnp.arange(BLOCKS_DEV, dtype=jnp.int32)[None, :]
    same_id = block_ids[..., :, None] == block_ids[..., None, :]
    position = lax.optimization_barrier(jnp.sum(same_id & earlier, axis=-1)).astype(jnp.int32)
    up_expert = up_weight[old_owner].astype(jnp.bfloat16)
    down_expert = down_weight[old_owner].astype(jnp.bfloat16)
    slots = jnp.arange(CAPACITY, dtype=jnp.int32)

    def one_rank(totals, members):
        rank_x, rank_dy, rank_ids, rank_pos = members
        rank_xf = rank_x.astype(jnp.float32)
        rank_dyf = rank_dy.astype(jnp.float32)

        def one_expert(gathered, expert):
            pick = ((rank_ids == expert)[:, None, :] & (rank_pos[:, None, :] == slots[None, :, None])).astype(jnp.float32)
            rows_x = jnp.einsum('erb,ebtd->ertd', pick, rank_xf).reshape(-1, D).astype(jnp.bfloat16)
            rows_dy = jnp.einsum('erb,ebtd->ertd', pick, rank_dyf).reshape(-1, D).astype(jnp.bfloat16)
            up_mat = up_expert[expert]
            down_mat = down_expert[expert]
            pre_act = jnp.dot(rows_x, up_mat, preferred_element_type=jnp.float32)
            active, slopes = silu_parts(pre_act)
            hidden = active.astype(jnp.bfloat16)
            back_grad = jnp.dot(rows_dy, down_mat.T, preferred_element_type=jnp.float32)
            pre_grad = (back_grad * slopes).astype(jnp.bfloat16)
            rows_grad = jnp.dot(pre_grad, up_mat.T, preferred_element_type=jnp.float32).astype(jnp.bfloat16)
            up_part = jnp.dot(rows_x.T, pre_grad, preferred_element_type=jnp.float32).astype(jnp.bfloat16)
            down_part = jnp.dot(hidden.T, rows_dy, preferred_element_type=jnp.float32).astype(jnp.bfloat16)
            placed = jnp.einsum('erb,ertd->ebtd', pick, rows_grad.reshape(groups, CAPACITY, BLOCK_TOK, D).astype(jnp.float32))
            return (gathered + placed, (up_part, down_part))
        start = jnp.zeros((groups, BLOCKS_DEV, BLOCK_TOK, D), jnp.float32)
        grads_here, parts = lax.scan(one_expert, start, jnp.arange(EXPERTS, dtype=jnp.int32))
        new_totals = (totals[0] + parts[0].astype(jnp.float32), totals[1] + parts[1].astype(jnp.float32))
        return (new_totals, grads_here.astype(jnp.bfloat16))
    init = (jnp.zeros((EXPERTS, D, FF), jnp.float32), jnp.zeros((EXPERTS, FF, D), jnp.float32))
    members = (inputs.transpose(1, 0, 2, 3, 4), upstream.transpose(1, 0, 2, 3, 4), block_ids.transpose(1, 0, 2), position.transpose(1, 0, 2))
    totals, grads_all = lax.scan(one_rank, init, members)
    token_grad = grads_all.transpose(1, 0, 2, 3, 4).reshape(TOKENS, D)
    up_new = adam_update(up_weight[old_owner], up_first[old_owner], up_second[old_owner], totals[0])
    down_new = adam_update(down_weight[old_owner], down_first[old_owner], down_second[old_owner], totals[1])
    incoming = jnp.zeros((EXPERTS,), jnp.int32).at[new_owner].set(jnp.arange(EXPERTS, dtype=jnp.int32))
    return (token_grad, up_new[0][incoming], down_new[0][incoming], up_new[1][incoming], up_new[2][incoming], down_new[1][incoming], down_new[2][incoming])
```

```python
import jax
import jax.numpy as jnp
from jax import lax
from jax.experimental import pallas as pl
from jax.experimental.pallas import tpu as pltpu
from jax.sharding import Mesh
from jax.sharding import PartitionSpec as P

beta_one = 0.9
beta_two = 0.95
bias_one = 1.0 - 0.9**10
bias_two = 1.0 - 0.95**10
rate_value = 0.01
decay_value = 0.1
eps_value = 1e-08

F32 = jnp.float32
BF = jnp.bfloat16
NX, NY, NC = 2, 4, 2
LANE = 128


def row_order():
    return [x * NY * NC + y * NC + c for c in range(NC) for y in range(NY) for x in range(NX)]


def inverse(order):
    back = [0] * len(order)
    for p, r in enumerate(order):
        back[r] = p
    return back


def lanes_taken(value, order):
    width = value.shape[1] // len(order)
    return jnp.concatenate([value[:, r * width : (r + 1) * width] for r in order], axis=1)


def cast_body(up_ref, down_ref, u_ref, w_ref):
    u_ref[...] = lanes_taken(up_ref[...], row_order()).astype(BF)
    w_ref[...] = down_ref[...].astype(BF)


def cast_weights(up, down):
    return pl.pallas_call(
        cast_body,
        out_shape=(jax.ShapeDtypeStruct(up.shape, BF), jax.ShapeDtypeStruct(down.shape, BF)),
        name="cast_weights",
    )(up, down)


def slot_of_block(ids_ref, own_ref, b):
    mine = ids_ref[b, 0]
    place = jnp.int32(0)
    for e in range(b):
        place = place + (ids_ref[e, 0] == mine).astype(jnp.int32)
    return own_ref[mine] * 2 + place


def dispatch_body(ids_ref, count_ref, own_ref, tok_ref, cot_ref, sx_ref, sdy_ref):
    blocks, rows, _ = tok_ref.shape
    sx_ref[...] = jnp.zeros(sx_ref.shape, BF)
    sdy_ref[...] = jnp.zeros(sdy_ref.shape, BF)
    at = lax.broadcasted_iota(jnp.int32, (rows, 1), 0)
    for b in range(blocks):
        slot = slot_of_block(ids_ref, own_ref, b)
        alive = at < count_ref[b]
        x = jnp.where(alive, tok_ref[b].astype(F32), 0.0)
        dy = jnp.where(alive, cot_ref[b].astype(F32), 0.0)
        sx_ref[slot] = lanes_taken(x, row_order()).astype(BF)
        sdy_ref[slot] = dy.astype(BF)


def smem():
    return pl.BlockSpec(memory_space=pltpu.SMEM)


def vmem():
    return pl.BlockSpec(memory_space=pltpu.VMEM)


def dispatch(ids, count, owner, tokens, cotangent):
    blocks, rows, width = tokens.shape
    out = jax.ShapeDtypeStruct((2 * blocks, rows, width), BF)
    return pl.pallas_call(
        dispatch_body,
        in_specs=[smem(), smem(), smem(), vmem(), vmem()],
        out_shape=(out, out),
        name="dispatch",
    )(ids, count, owner, tokens, cotangent)


def combine_body(ids_ref, own_ref, ret_ref, out_ref):
    for b in range(out_ref.shape[0]):
        slot = slot_of_block(ids_ref, own_ref, b)
        out_ref[b] = lanes_taken(ret_ref[slot].astype(F32), inverse(row_order())).astype(BF)


def combine(ids, owner, returned):
    slots, rows, width = returned.shape
    return pl.pallas_call(
        combine_body,
        in_specs=[smem(), smem(), vmem()],
        out_shape=jax.ShapeDtypeStruct((slots // 2, rows, width), BF),
        name="combine",
    )(ids, owner, returned)


def to_tiles(rows8):
    n = rows8.shape[1] // LANE
    return jnp.concatenate([rows8[:, i * LANE : (i + 1) * LANE] for i in range(n)], axis=0)


def from_tiles(tiles):
    n = tiles.shape[0] // 8
    return jnp.concatenate([tiles[i * 8 : (i + 1) * 8] for i in range(n)], axis=1)


def pack_body(a_ref, b_ref, c_ref, d_ref, e_ref, f_ref, out_ref):
    for i, ref in enumerate((a_ref, b_ref, c_ref)):
        out_ref[0, i] = ref[...].astype(BF)
    for i, ref in enumerate((d_ref, e_ref, f_ref)):
        out_ref[0, 3 + i] = to_tiles(ref[...]).astype(BF)


def pack_states(ups, downs, groups):
    rows, cols = ups[0].shape
    drows, dcols = downs[0].shape
    wide, tall = cols // groups, drows // groups
    up_spec = pl.BlockSpec((rows, wide), lambda i: (0, i))
    down_spec = pl.BlockSpec((tall, dcols), lambda i: (i, 0))
    return pl.pallas_call(
        pack_body,
        grid=(groups,),
        in_specs=[up_spec] * 3 + [down_spec] * 3,
        out_specs=pl.BlockSpec((1, 6, rows, wide), lambda i: (i, 0, 0, 0)),
        out_shape=jax.ShapeDtypeStruct((groups, 6, rows, wide), BF),
        name="pack_states",
    )(*ups, *downs)


def order_body(source_ref, in_ref, out_ref):
    out_ref[...] = in_ref[...]


def order_states(source, shares):
    groups, rest = shares.shape[0], shares.shape[1:]
    zeros = (0,) * len(rest)
    return pl.pallas_call(
        order_body,
        grid_spec=pltpu.PrefetchScalarGridSpec(
            num_scalar_prefetch=1,
            grid=(groups,),
            in_specs=[pl.BlockSpec((1,) + rest, lambda i, s: (s[i],) + zeros)],
            out_specs=pl.BlockSpec((1,) + rest, lambda i, s: (i,) + zeros),
        ),
        out_shape=jax.ShapeDtypeStruct(shares.shape, BF),
        name="order_states",
    )(source, shares)


def sum_body(source_ref, in_ref, out_ref):
    both = in_ref[0].astype(F32)
    out_ref[0] = (both[0] + both[1]).astype(BF)


def sum_order(source, shares):
    groups, pair, rows, wide = shares.shape
    return pl.pallas_call(
        sum_body,
        grid_spec=pltpu.PrefetchScalarGridSpec(
            num_scalar_prefetch=1,
            grid=(groups,),
            in_specs=[pl.BlockSpec((1, pair, rows, wide), lambda i, s: (s[i], 0, 0, 0))],
            out_specs=pl.BlockSpec((1, rows, wide), lambda i, s: (i, 0, 0)),
        ),
        out_shape=jax.ShapeDtypeStruct((groups, rows, wide), BF),
        name="sum_order",
    )(source, shares)


def weight_grad_body(half_ref, a_ref, ao_ref, b_ref, bo_ref, out_ref):
    dims = (((0,), (0,)), ((), ()))
    total = lax.dot_general(a_ref[...], b_ref[...], dims, preferred_element_type=F32)
    total += lax.dot_general(ao_ref[...], bo_ref[...], dims, preferred_element_type=F32)
    out_ref[...] = total.astype(BF)


def weight_grad(half, a, a_other, b, b_other, step, name):
    rows, width = a.shape
    cols = b.shape[1]
    steps = width // 2 // step
    left = pl.BlockSpec((rows, step), lambda i, h: (0, h[0] * steps + i))
    right = pl.BlockSpec((rows, cols), lambda i, h: (0, 0))
    return pl.pallas_call(
        weight_grad_body,
        grid_spec=pltpu.PrefetchScalarGridSpec(
            num_scalar_prefetch=1,
            grid=(steps,),
            in_specs=[left, left, right, right],
            out_specs=pl.BlockSpec((step, cols), lambda i, h: (i, 0)),
        ),
        out_shape=jax.ShapeDtypeStruct((width // 2, cols), BF),
        name=name,
    )(half, a, a_other, b, b_other)


def pack_up_body(in_ref, out_ref):
    value = lanes_taken(in_ref[0].astype(F32), inverse(row_order())).astype(BF)
    for i in range(out_ref.shape[0]):
        out_ref[i, 0] = value[:, i * LANE : (i + 1) * LANE]


def pack_up_grad(grad, groups):
    pair, rows, cols = grad.shape
    wide = cols // groups
    return pl.pallas_call(
        pack_up_body,
        grid=(pair,),
        in_specs=[pl.BlockSpec((1, rows, cols), lambda i: (i, 0, 0))],
        out_specs=pl.BlockSpec((groups, 1, rows, wide), lambda i: (0, i, 0, 0)),
        out_shape=jax.ShapeDtypeStruct((groups, pair, rows, wide), BF),
        name="pack_up_grad",
    )(grad)


def pack_down_body(in_ref, out_ref):
    for i in range(out_ref.shape[0]):
        out_ref[i, 0] = to_tiles(in_ref[0, i * 8 : (i + 1) * 8].astype(F32)).astype(BF)


def pack_down_grad(grad, groups):
    pair, rows, cols = grad.shape
    tall = rows // groups * cols // LANE
    return pl.pallas_call(
        pack_down_body,
        grid=(pair,),
        in_specs=[pl.BlockSpec((1, rows, cols), lambda i: (i, 0, 0))],
        out_specs=pl.BlockSpec((groups, 1, tall, LANE), lambda i: (0, i, 0, 0)),
        out_shape=jax.ShapeDtypeStruct((groups, pair, tall, LANE), BF),
        name="pack_down_grad",
    )(grad)


def adam_update(weight, moment, second, gradient):
    moment_new = beta_one * moment + (1.0 - beta_one) * gradient
    second_new = beta_two * second + (1.0 - beta_two) * gradient * gradient
    update = moment_new / bias_one / (jnp.sqrt(second_new / bias_two) + eps_value)
    return (weight - rate_value * (update + decay_value * weight), moment_new, second_new)


def adam_up_body(state_ref, grad_ref, w_ref, m_ref, v_ref):
    w, m, v = (state_ref[0, i].astype(F32) for i in range(3))
    w_ref[...], m_ref[...], v_ref[...] = adam_update(w, m, v, grad_ref[0].astype(F32))


def adam_down_body(state_ref, grad_ref, w_ref, m_ref, v_ref):
    w, m, v = (state_ref[0, i].astype(F32) for i in range(3))
    new = adam_update(w, m, v, grad_ref[0].astype(F32))
    for ref, value in zip((w_ref, m_ref, v_ref), new):
        ref[...] = from_tiles(value)


def adam(body, states, which, grad, out_block, out_index, out_shape, name):
    groups, _, rows, wide = states.shape
    out_spec = pl.BlockSpec(out_block, out_index)
    return pl.pallas_call(
        body,
        grid=(groups,),
        in_specs=[
            pl.BlockSpec((1, 3, rows, wide), lambda i: (i, which, 0, 0)),
            pl.BlockSpec((1, rows, wide), lambda i: (i, 0, 0)),
        ],
        out_specs=[out_spec] * 3,
        out_shape=[jax.ShapeDtypeStruct(out_shape, F32)] * 3,
        name=name,
    )(states, grad)


def silu_parts(pre_act):
    sigma = jax.nn.sigmoid(pre_act)
    return (pre_act * sigma, sigma * (1.0 + pre_act * (1.0 - sigma)))


def exchange(array, axis):
    return lax.all_to_all(array, axis, split_axis=0, concat_axis=0, tiled=True)


def from_partner(array):
    return lax.ppermute(array, "core", [(0, 1), (1, 0)])


def local(
    tokens,
    cotangent,
    block_expert,
    block_count,
    old_owner,
    new_owner,
    up_weight,
    down_weight,
    up_first,
    up_second,
    down_first,
    down_second,
):
    groups = lax.axis_size("expert")
    tok_rows, features = tokens.shape
    blocks = block_count.shape[0]
    rows = tok_rows // blocks
    labels = jnp.arange(groups, dtype=jnp.int32)
    incoming = jnp.sum(jnp.where(new_owner[:, None] == labels[None, :], labels[:, None], 0), axis=0)
    source = jnp.sum(jnp.where(labels[:, None] == incoming[None, :], old_owner[:, None], 0), axis=0)
    half = lax.axis_index("core").astype(jnp.int32).reshape(1)

    up_short, down_short = cast_weights(up_weight[0], down_weight[0])
    up_pair = lax.all_gather(up_short, "x", axis=0, tiled=True)
    up_mat = lax.all_gather(up_pair, ("core", "y"), axis=0, tiled=True)
    down_pair = lax.all_gather(down_short, "x", axis=0, tiled=True)
    down_mat = lax.all_gather(down_pair, ("core", "y"), axis=0, tiled=True)

    send_x, send_dy = dispatch(
        block_expert,
        block_count,
        old_owner,
        tokens.reshape(blocks, rows, features),
        cotangent.reshape(blocks, rows, features),
    )
    send_x, send_dy, _ = lax.optimization_barrier((send_x, send_dy, down_pair))
    inputs = exchange(send_x, "expert").reshape(-1, features)
    upstream = exchange(send_dy, "expert").reshape(-1, features)
    inputs_other, upstream_other = from_partner(inputs), from_partner(upstream)

    packed = pack_states(
        (up_weight[0], up_first[0], up_second[0]),
        (down_weight[0], down_first[0], down_second[0]),
        groups,
    )
    packed, _ = lax.optimization_barrier((packed, upstream))
    shares = exchange(packed, "expert")

    pre_act = jnp.dot(inputs, up_mat, preferred_element_type=F32)
    active, slopes = silu_parts(pre_act)
    hidden = active.astype(BF)
    hidden_other = from_partner(hidden)
    down_part = weight_grad(
        half, hidden, hidden_other, upstream, upstream_other, 128, "down_part"
    )
    down_sum = lax.psum_scatter(down_part, "y", scatter_dimension=0, tiled=True)
    back = lax.dot_general(upstream, down_mat, (((1,), (1,)), ((), ())), preferred_element_type=F32)
    pre_grad = (back * slopes).astype(BF)
    pre_grad_other = from_partner(pre_grad)
    up_part = weight_grad(half, inputs, inputs_other, pre_grad, pre_grad_other, 256, "up_part")
    up_sum = lax.psum_scatter(up_part, "y", scatter_dimension=0, tiled=True)
    input_grad = lax.dot_general(
        pre_grad, up_mat, (((1,), (1,)), ((), ())), preferred_element_type=F32
    ).astype(BF)

    ordered = order_states(source, shares)
    ordered, _ = lax.optimization_barrier((ordered, up_part))
    states = exchange(ordered, "expert")

    returned = exchange(input_grad.reshape(-1, rows, features), "expert")
    token_grad = combine(block_expert, old_owner, returned).reshape(tok_rows, features)

    def moved(packed_grad):
        shape = packed_grad.shape
        spread = exchange(packed_grad.reshape((-1,) + shape[2:]), ("expert", "x"))
        return exchange(sum_order(source, spread.reshape(shape)), "expert")

    down_grad = moved(pack_down_grad(down_sum.reshape(NX, -1, features), groups))
    up_grad = moved(pack_up_grad(up_sum.reshape(NX, -1, up_mat.shape[1]), groups))

    up_shape, down_shape = up_weight.shape[1:], down_weight.shape[1:]
    down_new = adam(
        adam_down_body, states, 1, down_grad,
        (down_shape[0] // groups, down_shape[1]), lambda i: (i, 0), down_shape, "adam_down",
    )
    up_new = adam(
        adam_up_body, states, 0, up_grad,
        (up_shape[0], up_shape[1] // groups), lambda i: (0, i), up_shape, "adam_up",
    )
    return (
        token_grad,
        up_new[0][None],
        down_new[0][None],
        up_new[1][None],
        up_new[2][None],
        down_new[1][None],
        down_new[2][None],
    )


def solution(mesh):
    fine = Mesh(
        mesh.devices.reshape(mesh.devices.shape[0], NX, NY, NC), ("expert", "x", "y", "core")
    )
    every = ("expert", "x", "y", "core")
    dp = ("x", "y", "core")
    state = P("expert", dp, None)
    return jax.shard_map(
        local,
        mesh=fine,
        in_specs=(P(every, None), P(every, None), P(every, None), P(every), P(), P())
        + (state,) * 6,
        out_specs=(P(every, None),) + (state,) * 6,
        check_vma=False,
    )
```

```python
import jax
import jax.numpy as jnp
from jax import lax
from jax.experimental import pallas as pl
from jax.experimental.pallas import tpu as pltpu
from jax.sharding import Mesh
from jax.sharding import PartitionSpec as P


beta_one = 0.9
beta_two = 0.95
bias_one = 1.0 - 0.9**10
bias_two = 1.0 - 0.95**10
rate_value = 0.01
decay_value = 0.1
eps_value = 1e-08

F32 = jnp.float32
BF = jnp.bfloat16
NX, NY, NC = 2, 4, 2
LANE = 128


def row_order():
    return [x * NY * NC + y * NC + c for c in range(NC) for y in range(NY) for x in range(NX)]


def inverse(order):
    back = [0] * len(order)
    for p, r in enumerate(order):
        back[r] = p
    return back


def lanes_taken(value, order):
    width = value.shape[1] // len(order)
    return jnp.concatenate([value[:, r * width : (r + 1) * width] for r in order], axis=1)


def cast_body(up_ref, down_ref, u_ref, w_ref):
    u_ref[...] = lanes_taken(up_ref[...], row_order()).astype(BF)
    w_ref[...] = down_ref[...].astype(BF)


def cast_weights(up, down):
    return pl.pallas_call(
        cast_body,
        out_shape=(jax.ShapeDtypeStruct(up.shape, BF), jax.ShapeDtypeStruct(down.shape, BF)),
        name="cast_weights",
    )(up, down)


def slot_of_block(ids_ref, own_ref, b):
    mine = ids_ref[b, 0]
    place = jnp.int32(0)
    for e in range(b):
        place = place + (ids_ref[e, 0] == mine).astype(jnp.int32)
    return own_ref[mine] * 2 + place


def dispatch_body(ids_ref, count_ref, own_ref, tok_ref, cot_ref, sx_ref, sdy_ref):
    blocks, rows, _ = tok_ref.shape
    sx_ref[...] = jnp.zeros(sx_ref.shape, BF)
    sdy_ref[...] = jnp.zeros(sdy_ref.shape, BF)
    at = lax.broadcasted_iota(jnp.int32, (rows, 1), 0)
    for b in range(blocks):
        slot = slot_of_block(ids_ref, own_ref, b)
        alive = at < count_ref[b]
        x = jnp.where(alive, tok_ref[b].astype(F32), 0.0)
        dy = jnp.where(alive, cot_ref[b].astype(F32), 0.0)
        sx_ref[slot] = lanes_taken(x, row_order()).astype(BF)
        sdy_ref[slot] = dy.astype(BF)


def smem():
    return pl.BlockSpec(memory_space=pltpu.SMEM)


def vmem():
    return pl.BlockSpec(memory_space=pltpu.VMEM)


def dispatch(ids, count, owner, tokens, cotangent):
    blocks, rows, width = tokens.shape
    out = jax.ShapeDtypeStruct((2 * blocks, rows, width), BF)
    return pl.pallas_call(
        dispatch_body,
        in_specs=[smem(), smem(), smem(), vmem(), vmem()],
        out_shape=(out, out),
        name="dispatch",
    )(ids, count, owner, tokens, cotangent)


def combine_body(ids_ref, own_ref, ret_ref, out_ref):
    for b in range(out_ref.shape[0]):
        slot = slot_of_block(ids_ref, own_ref, b)
        out_ref[b] = lanes_taken(ret_ref[slot].astype(F32), inverse(row_order())).astype(BF)


def combine(ids, owner, returned):
    slots, rows, width = returned.shape
    return pl.pallas_call(
        combine_body,
        in_specs=[smem(), smem(), vmem()],
        out_shape=jax.ShapeDtypeStruct((slots // 2, rows, width), BF),
        name="combine",
    )(ids, owner, returned)


def to_tiles(rows8):
    n = rows8.shape[1] // LANE
    return jnp.concatenate([rows8[:, i * LANE : (i + 1) * LANE] for i in range(n)], axis=0)


def from_tiles(tiles):
    n = tiles.shape[0] // 8
    return jnp.concatenate([tiles[i * 8 : (i + 1) * 8] for i in range(n)], axis=1)


def pack_body(a_ref, b_ref, c_ref, d_ref, e_ref, f_ref, out_ref):
    for g in range(out_ref.shape[0]):
        for i, ref in enumerate((a_ref, b_ref, c_ref)):
            out_ref[g, i] = ref[:, g * LANE : (g + 1) * LANE].astype(BF)
        for i, ref in enumerate((d_ref, e_ref, f_ref)):
            out_ref[g, 3 + i] = to_tiles(ref[g * 8 : (g + 1) * 8]).astype(BF)


def pack_states(ups, downs, groups):
    rows, cols = ups[0].shape
    return pl.pallas_call(
        pack_body,
        out_shape=jax.ShapeDtypeStruct((groups, 6, rows, cols // groups), BF),
        name="pack_states",
    )(*ups, *downs)


def order_body(source_ref, in_ref, out_ref):
    for g in range(out_ref.shape[0]):
        out_ref[g] = in_ref[source_ref[g]]


def order_states(source, shares):
    return pl.pallas_call(
        order_body,
        in_specs=[smem(), vmem()],
        out_shape=jax.ShapeDtypeStruct(shares.shape, BF),
        name="order_states",
    )(source, shares)


def sum_body(source_ref, in_ref, out_ref):
    for g in range(out_ref.shape[0]):
        both = in_ref[source_ref[g]].astype(F32)
        out_ref[g] = (both[0] + both[1]).astype(BF)


def sum_order(source, shares):
    groups, _, rows, wide = shares.shape
    return pl.pallas_call(
        sum_body,
        in_specs=[smem(), vmem()],
        out_shape=jax.ShapeDtypeStruct((groups, rows, wide), BF),
        name="sum_order",
    )(source, shares)


def weight_grad_body(half_ref, a_ref, ao_ref, b_ref, bo_ref, out_ref):
    dims = (((0,), (0,)), ((), ()))
    total = lax.dot_general(a_ref[...], b_ref[...], dims, preferred_element_type=F32)
    total += lax.dot_general(ao_ref[...], bo_ref[...], dims, preferred_element_type=F32)
    out_ref[...] = total.astype(BF)


def weight_grad(half, a, a_other, b, b_other, step):
    rows, width = a.shape
    cols = b.shape[1]
    steps = width // 2 // step
    left = pl.BlockSpec((rows, step), lambda i, h: (0, h[0] * steps + i))
    right = pl.BlockSpec((rows, cols), lambda i, h: (0, 0))
    return pl.pallas_call(
        weight_grad_body,
        grid_spec=pltpu.PrefetchScalarGridSpec(
            num_scalar_prefetch=1,
            grid=(steps,),
            in_specs=[left, left, right, right],
            out_specs=pl.BlockSpec((step, cols), lambda i, h: (i, 0)),
        ),
        out_shape=jax.ShapeDtypeStruct((width // 2, cols), BF),
    )(half, a, a_other, b, b_other)


def pack_up_body(in_ref, out_ref):
    for x in range(in_ref.shape[0]):
        value = lanes_taken(in_ref[x].astype(F32), inverse(row_order())).astype(BF)
        for i in range(out_ref.shape[0]):
            out_ref[i, x] = value[:, i * LANE : (i + 1) * LANE]


def pack_down_body(in_ref, out_ref):
    for x in range(in_ref.shape[0]):
        for i in range(out_ref.shape[0]):
            out_ref[i, x] = to_tiles(in_ref[x, i * 8 : (i + 1) * 8].astype(F32)).astype(BF)


def pack_grad(body, grad, groups):
    pair, rows, cols = grad.shape
    return pl.pallas_call(
        body,
        out_shape=jax.ShapeDtypeStruct((groups, pair, rows * cols // groups // LANE, LANE), BF),
    )(grad)


def adam_update(weight, moment, second, gradient):
    moment_new = beta_one * moment + (1.0 - beta_one) * gradient
    second_new = beta_two * second + (1.0 - beta_two) * gradient * gradient
    update = moment_new / bias_one / (jnp.sqrt(second_new / bias_two) + eps_value)
    return (weight - rate_value * (update + decay_value * weight), moment_new, second_new)


def adam_share(state_ref, grad_ref, g):
    w, m, v = (state_ref[g, i].astype(F32) for i in range(3))
    return adam_update(w, m, v, grad_ref[g].astype(F32))


def adam_up_body(state_ref, grad_ref, *outs):
    for g in range(grad_ref.shape[0]):
        for ref, value in zip(outs, adam_share(state_ref, grad_ref, g)):
            ref[:, g * LANE : (g + 1) * LANE] = value


def adam_down_body(state_ref, grad_ref, *outs):
    for g in range(grad_ref.shape[0]):
        for ref, value in zip(outs, adam_share(state_ref, grad_ref, g)):
            ref[g * 8 : (g + 1) * 8] = from_tiles(value)


def adam(body, states, which, grad, shape):
    groups, _, rows, wide = states.shape
    full = pl.BlockSpec(shape, lambda i: (0, 0))
    return pl.pallas_call(
        body,
        grid=(1,),
        in_specs=[
            pl.BlockSpec((groups, 3, rows, wide), lambda i: (0, which, 0, 0)),
            pl.BlockSpec((groups, rows, wide), lambda i: (0, 0, 0)),
        ],
        out_specs=[full] * 3,
        out_shape=[jax.ShapeDtypeStruct(shape, F32)] * 3,
    )(states, grad)


def silu_parts(pre_act):
    sigma = jax.nn.sigmoid(pre_act)
    return (pre_act * sigma, sigma * (1.0 + pre_act * (1.0 - sigma)))


def exchange(array, axis):
    return lax.all_to_all(array, axis, split_axis=0, concat_axis=0, tiled=True)


def from_partner(array):
    return lax.ppermute(array, "core", [(0, 1), (1, 0)])


def step(
    tokens,
    cotangent,
    block_expert,
    block_count,
    old_owner,
    new_owner,
    up_weight,
    down_weight,
    up_first,
    up_second,
    down_first,
    down_second,
):
    groups = lax.axis_size("expert")
    tok_rows, features = tokens.shape
    blocks = block_count.shape[0]
    rows = tok_rows // blocks
    labels = jnp.arange(groups, dtype=jnp.int32)
    incoming = jnp.sum(jnp.where(new_owner[:, None] == labels[None, :], labels[:, None], 0), axis=0)
    source = jnp.sum(jnp.where(labels[:, None] == incoming[None, :], old_owner[:, None], 0), axis=0)
    half = lax.axis_index("core").astype(jnp.int32).reshape(1)

    up_short, down_short = cast_weights(up_weight[0], down_weight[0])
    up_mat = lax.all_gather(up_short, ("core", "y", "x"), axis=0, tiled=True)
    down_pair = lax.all_gather(down_short, "x", axis=0, tiled=True)
    down_mat = lax.all_gather(down_pair, ("core", "y"), axis=0, tiled=True)

    packed = pack_states(
        (up_weight[0], up_first[0], up_second[0]),
        (down_weight[0], down_first[0], down_second[0]),
        groups,
    )
    packed, _ = lax.optimization_barrier((packed, down_pair))
    shares = exchange(packed, "expert")

    send_x, send_dy = dispatch(
        block_expert,
        block_count,
        old_owner,
        tokens.reshape(blocks, rows, features),
        cotangent.reshape(blocks, rows, features),
    )
    send_x, shares = lax.optimization_barrier((send_x, shares))
    inputs = exchange(send_x, "expert")
    send_dy, inputs = lax.optimization_barrier((send_dy, inputs))
    inputs = inputs.reshape(-1, features)
    upstream = exchange(send_dy, "expert").reshape(-1, features)
    inputs_other, upstream_other = from_partner(inputs), from_partner(upstream)

    ordered = order_states(source, shares)
    ordered, upstream = lax.optimization_barrier((ordered, upstream))
    states = exchange(ordered, "expert")

    pre_act = jnp.dot(inputs, up_mat, preferred_element_type=F32)
    active, slopes = silu_parts(pre_act)
    hidden = active.astype(BF)
    hidden_other = from_partner(hidden)
    down_part = weight_grad(half, hidden, hidden_other, upstream, upstream_other, 128)
    down_sum = lax.psum_scatter(down_part, "y", scatter_dimension=0, tiled=True)
    upstream, _ = lax.optimization_barrier((upstream, down_part))
    back = lax.dot_general(upstream, down_mat, (((1,), (1,)), ((), ())), preferred_element_type=F32)
    pre_grad = (back * slopes).astype(BF)
    pre_grad_other = from_partner(pre_grad)
    up_part = weight_grad(half, inputs, inputs_other, pre_grad, pre_grad_other, 256)
    up_sum = lax.psum_scatter(up_part, "y", scatter_dimension=0, tiled=True)
    pre_grad, up_part = lax.optimization_barrier((pre_grad, up_part))
    input_grad = lax.dot_general(
        pre_grad, up_mat, (((1,), (1,)), ((), ())), preferred_element_type=F32
    ).astype(BF)
    input_grad, states = lax.optimization_barrier((input_grad, states))
    returned = exchange(input_grad.reshape(-1, rows, features), "expert")
    token_grad = combine(block_expert, old_owner, returned).reshape(tok_rows, features)

    def moved(packed_grad):
        shape = packed_grad.shape
        spread = exchange(packed_grad.reshape((-1,) + shape[2:]), ("expert", "x"))
        ordered_grad = sum_order(source, spread.reshape(shape))
        return exchange(ordered_grad, "expert")

    up_shape, down_shape = up_weight.shape[1:], down_weight.shape[1:]
    down_packed = pack_grad(pack_down_body, down_sum.reshape(NX, -1, features), groups)
    down_grad = moved(down_packed)
    down_new = adam(adam_down_body, states, 1, down_grad, down_shape)

    up_sum, down_new, token_grad = lax.optimization_barrier((up_sum, down_new, token_grad))
    up_packed = pack_grad(pack_up_body, up_sum.reshape(NX, -1, up_shape[1]), groups)
    up_grad = moved(up_packed)
    up_new = adam(adam_up_body, states, 0, up_grad, up_shape)
    return (
        token_grad,
        up_new[0][None],
        down_new[0][None],
        up_new[1][None],
        up_new[2][None],
        down_new[1][None],
        down_new[2][None],
    )


def solution(mesh):
    fine = Mesh(
        mesh.devices.reshape(mesh.devices.shape[0], NX, NY, NC), ("expert", "x", "y", "core")
    )
    every = ("expert", "x", "y", "core")
    dp = ("x", "y", "core")
    state = P("expert", dp, None)
    return jax.shard_map(
        step,
        mesh=fine,
        in_specs=(P(every, None), P(every, None), P(every, None), P(every), P(), P())
        + (state,) * 6,
        out_specs=(P(every, None),) + (state,) * 6,
        check_vma=False,
    )
```

```python
import jax
import jax.numpy as jnp
from jax import lax
from jax.experimental import pallas as pl
from jax.experimental.pallas import tpu as pltpu
from jax.sharding import Mesh
from jax.sharding import PartitionSpec as P


beta_one = 0.9
beta_two = 0.95
bias_one = 1.0 - 0.9**10
bias_two = 1.0 - 0.95**10
rate_value = 0.01
decay_value = 0.1
eps_value = 1e-08

F32 = jnp.float32
BF = jnp.bfloat16
NX, NY, NC = 2, 4, 2
LANE = 128


def row_order():
    return [x * NY * NC + y * NC + c for c in range(NC) for y in range(NY) for x in range(NX)]


def inverse(order):
    back = [0] * len(order)
    for p, r in enumerate(order):
        back[r] = p
    return back


def lanes_taken(value, order):
    width = value.shape[1] // len(order)
    return jnp.concatenate([value[:, r * width : (r + 1) * width] for r in order], axis=1)


def pack_weights_body(up_ref, down_ref, u_ref, w_ref):
    for g in range(u_ref.shape[0]):
        u_ref[g] = up_ref[:, g * LANE : (g + 1) * LANE].astype(BF)
        w_ref[g] = down_ref[g * 8 : (g + 1) * 8].astype(BF)


def pack_weights(up, down, groups):
    return pl.pallas_call(
        pack_weights_body,
        out_shape=(
            jax.ShapeDtypeStruct((groups, up.shape[0], LANE), BF),
            jax.ShapeDtypeStruct((groups, down.shape[0] // groups, down.shape[1]), BF),
        ),
        name="pack_weights",
    )(up, down)


def unpack_up_body(in_ref, out_ref):
    groups = in_ref.shape[0] // NX
    rows = in_ref.shape[1]
    for x in range(NX):
        value = jnp.concatenate([in_ref[g * NX + x].astype(F32) for g in range(groups)], axis=1)
        out_ref[x * rows : (x + 1) * rows] = lanes_taken(value, row_order()).astype(BF)


def unpack_down_body(in_ref, out_ref):
    groups = in_ref.shape[0] // NX
    rows = in_ref.shape[1]
    for x in range(NX):
        value = jnp.concatenate([in_ref[g * NX + x].astype(F32) for g in range(groups)], axis=0)
        out_ref[x * groups * rows : (x + 1) * groups * rows] = value.astype(BF)


def unpack(body, shares, shape):
    return pl.pallas_call(body, out_shape=jax.ShapeDtypeStruct(shape, BF))(shares)


def slot_of_block(ids_ref, own_ref, b):
    mine = ids_ref[b, 0]
    place = jnp.int32(0)
    for e in range(b):
        place = place + (ids_ref[e, 0] == mine).astype(jnp.int32)
    return own_ref[mine] * 2 + place


def dispatch_body(ids_ref, count_ref, own_ref, tok_ref, cot_ref, sx_ref, sdy_ref):
    blocks, rows, _ = tok_ref.shape
    sx_ref[...] = jnp.zeros(sx_ref.shape, BF)
    sdy_ref[...] = jnp.zeros(sdy_ref.shape, BF)
    at = lax.broadcasted_iota(jnp.int32, (rows, 1), 0)
    for b in range(blocks):
        slot = slot_of_block(ids_ref, own_ref, b)
        alive = at < count_ref[b]
        x = jnp.where(alive, tok_ref[b].astype(F32), 0.0)
        dy = jnp.where(alive, cot_ref[b].astype(F32), 0.0)
        sx_ref[slot] = lanes_taken(x, row_order()).astype(BF)
        sdy_ref[slot] = dy.astype(BF)


def smem():
    return pl.BlockSpec(memory_space=pltpu.SMEM)


def vmem():
    return pl.BlockSpec(memory_space=pltpu.VMEM)


def dispatch(ids, count, owner, tokens, cotangent):
    blocks, rows, width = tokens.shape
    out = jax.ShapeDtypeStruct((2 * blocks, rows, width), BF)
    return pl.pallas_call(
        dispatch_body,
        in_specs=[smem(), smem(), smem(), vmem(), vmem()],
        out_shape=(out, out),
        name="dispatch",
    )(ids, count, owner, tokens, cotangent)


def combine_body(ids_ref, own_ref, ret_ref, out_ref):
    for b in range(out_ref.shape[0]):
        slot = slot_of_block(ids_ref, own_ref, b)
        out_ref[b] = lanes_taken(ret_ref[slot].astype(F32), inverse(row_order())).astype(BF)


def combine(ids, owner, returned):
    slots, rows, width = returned.shape
    return pl.pallas_call(
        combine_body,
        in_specs=[smem(), smem(), vmem()],
        out_shape=jax.ShapeDtypeStruct((slots // 2, rows, width), BF),
        name="combine",
    )(ids, owner, returned)


def to_tiles(rows8):
    n = rows8.shape[1] // LANE
    return jnp.concatenate([rows8[:, i * LANE : (i + 1) * LANE] for i in range(n)], axis=0)


def from_tiles(tiles):
    n = tiles.shape[0] // 8
    return jnp.concatenate([tiles[i * 8 : (i + 1) * 8] for i in range(n)], axis=1)


def pack_body(a_ref, b_ref, c_ref, d_ref, out_ref):
    for g in range(out_ref.shape[0]):
        for i, ref in enumerate((a_ref, b_ref)):
            out_ref[g, i] = ref[:, g * LANE : (g + 1) * LANE].astype(BF)
        for i, ref in enumerate((c_ref, d_ref)):
            out_ref[g, 2 + i] = to_tiles(ref[g * 8 : (g + 1) * 8]).astype(BF)


def pack_states(ups, downs, groups):
    rows, cols = ups[0].shape
    return pl.pallas_call(
        pack_body,
        out_shape=jax.ShapeDtypeStruct((groups, 4, rows, cols // groups), BF),
        name="pack_states",
    )(*ups, *downs)


def order_body(old_ref, new_ref, in_ref, out_ref):
    copies = out_ref.shape[0] // in_ref.shape[0]
    for k in range(in_ref.shape[0]):
        for i in range(copies):
            out_ref[new_ref[k] * copies + i] = in_ref[old_ref[k]]


def order_states(old, new, shares, copies):
    shape = (shares.shape[0] * copies,) + shares.shape[1:]
    return pl.pallas_call(
        order_body, in_specs=[smem(), smem(), vmem()], out_shape=jax.ShapeDtypeStruct(shape, BF)
    )(old, new, shares)


def weight_grad_body(half_ref, a_ref, ao_ref, b_ref, bo_ref, out_ref):
    dims = (((0,), (0,)), ((), ()))
    total = lax.dot_general(a_ref[...], b_ref[...], dims, preferred_element_type=F32)
    total += lax.dot_general(ao_ref[...], bo_ref[...], dims, preferred_element_type=F32)
    out_ref[...] = total.astype(BF)


def weight_grad(place, a, a_other, b, b_other, step):
    rows, width = a.shape
    cols = b.shape[1]
    steps = width // 2 // step
    left = pl.BlockSpec(
        (rows, step), lambda i, at: (0, at[0] * steps + lax.rem(at[1] + i, steps))
    )
    right = pl.BlockSpec((rows, cols), lambda i, at: (0, 0))
    return pl.pallas_call(
        weight_grad_body,
        grid_spec=pltpu.PrefetchScalarGridSpec(
            num_scalar_prefetch=1,
            grid=(steps,),
            in_specs=[left, left, right, right],
            out_specs=pl.BlockSpec((step, cols), lambda i, at: (i, 0)),
        ),
        out_shape=jax.ShapeDtypeStruct((width // 2, cols), BF),
    )(place, a, a_other, b, b_other)


def relay_body(part_ref, below_ref, above_ref, up_ref, down_ref):
    tall = below_ref.shape[0]
    wide = 2 * tall
    mine = part_ref[wide : 2 * wide].astype(F32)
    up_ref[0:tall] = (mine[0:tall] + below_ref[...].astype(F32)).astype(BF)
    up_ref[tall:wide] = part_ref[wide + tall : 2 * wide]
    mine = part_ref[3 * wide + tall : 4 * wide].astype(F32)
    down_ref[0:tall] = part_ref[3 * wide : 3 * wide + tall]
    down_ref[tall:wide] = (mine + above_ref[...].astype(F32)).astype(BF)


def relay(part, below, above):
    tall, cols = below.shape
    out = jax.ShapeDtypeStruct((2 * tall, cols), BF)
    return pl.pallas_call(relay_body, out_shape=(out, out), name="relay")(part, below, above)


def finish_body(x_ref, part_ref, below_ref, above_ref, own_ref, send_ref):
    tall = own_ref.shape[0]
    total = part_ref[...].astype(F32) + below_ref[...].astype(F32) + above_ref[...].astype(F32)
    low, high = total[0:tall], total[tall : 2 * tall]
    first = x_ref[0] == 0
    own_ref[...] = jnp.where(first, low, high)
    send_ref[...] = jnp.where(first, high, low).astype(BF)


def finish(x_at, part, below, above):
    wide, cols = below.shape
    whole = pl.BlockSpec((wide, cols), lambda i: (0, 0))
    half_spec = pl.BlockSpec((wide // 2, cols), lambda i: (0, 0))
    return pl.pallas_call(
        finish_body,
        grid=(1,),
        in_specs=[smem(), whole, whole, whole],
        out_specs=(half_spec, half_spec),
        out_shape=(
            jax.ShapeDtypeStruct((wide // 2, cols), F32),
            jax.ShapeDtypeStruct((wide // 2, cols), BF),
        ),
        name="finish",
    )(x_at, part, below, above)


def adam_update(weight, moment, second, gradient):
    moment_new = beta_one * moment + (1.0 - beta_one) * gradient
    second_new = beta_two * second + (1.0 - beta_two) * gradient * gradient
    update = moment_new / bias_one / (jnp.sqrt(second_new / bias_two) + eps_value)
    return (weight - rate_value * (update + decay_value * weight), moment_new, second_new)


def adam_up_body(x_ref, weight_ref, state_ref, grad_ref, *outs):
    grad = lanes_taken(grad_ref[...].astype(F32), inverse(row_order()))
    for g in range(state_ref.shape[0]):
        lanes = slice(g * LANE, (g + 1) * LANE)
        m, v = (state_ref[g, i].astype(F32) for i in range(2))
        w = weight_ref[g * NX + x_ref[0]].astype(F32)
        for ref, value in zip(outs, adam_update(w, m, v, grad[:, lanes])):
            ref[:, lanes] = value


def adam_down_body(x_ref, weight_ref, state_ref, grad_ref, other_ref, *outs):
    for g in range(state_ref.shape[0]):
        rows = slice(g * 8, (g + 1) * 8)
        m, v = (from_tiles(state_ref[g, i].astype(F32)) for i in range(2))
        w = weight_ref[g * NX + x_ref[0]].astype(F32)
        grad = grad_ref[rows] + other_ref[rows].astype(F32)
        for ref, value in zip(outs, adam_update(w, m, v, grad)):
            ref[rows] = value


def adam(body, x_at, weights, states, which, grads, shape):
    groups, _, rows, wide = states.shape
    full = pl.BlockSpec(shape, lambda i: (0, 0))
    return pl.pallas_call(
        body,
        grid=(1,),
        in_specs=[
            smem(),
            pl.BlockSpec(weights.shape, lambda i: (0, 0, 0)),
            pl.BlockSpec((groups, 2, rows, wide), lambda i: (0, which, 0, 0)),
        ]
        + [full] * len(grads),
        out_specs=[full] * 3,
        out_shape=[jax.ShapeDtypeStruct(shape, F32)] * 3,
    )(x_at, weights, states, *grads)


def silu_parts(pre_act):
    sigma = jax.nn.sigmoid(pre_act)
    return (pre_act * sigma, sigma * (1.0 + pre_act * (1.0 - sigma)))


def exchange(array, axis):
    return lax.all_to_all(array, axis, split_axis=0, concat_axis=0, tiled=True)


def from_partner(array):
    return lax.ppermute(array, "core", [(0, 1), (1, 0)])


def step(
    tokens,
    cotangent,
    block_expert,
    block_count,
    old_owner,
    new_owner,
    up_weight,
    down_weight,
    up_first,
    up_second,
    down_first,
    down_second,
):
    groups = lax.axis_size("expert")
    tok_rows, features = tokens.shape
    blocks = block_count.shape[0]
    rows = tok_rows // blocks
    core_at = lax.axis_index("core").astype(jnp.int32)
    y_at = lax.axis_index("y").astype(jnp.int32)
    x_at = lax.axis_index("x").astype(jnp.int32).reshape(1)
    up_place = jnp.stack([core_at, jnp.zeros((), jnp.int32)])
    down_place = jnp.stack([core_at, y_at])
    up_shape, down_shape = up_weight.shape[1:], down_weight.shape[1:]

    up_packed, down_packed = pack_weights(up_weight[0], down_weight[0], groups)

    def weight_moved(packed):
        spread = exchange(packed, "expert")
        ordered = order_states(old_owner, new_owner, spread, NX)
        return exchange(ordered, ("expert", "x"))

    up_shares = weight_moved(up_packed)
    up_pair = unpack(unpack_up_body, up_shares, (NX * up_shape[0], up_shape[1]))
    up_mat = lax.all_gather(up_pair, ("core", "y"), axis=0, tiled=True)

    down_packed, up_pair = lax.optimization_barrier((down_packed, up_pair))
    down_shares = weight_moved(down_packed)
    down_pair = unpack(unpack_down_body, down_shares, (NX * down_shape[0], down_shape[1]))
    down_mat = lax.all_gather(down_pair, ("core", "y"), axis=0, tiled=True)

    send_x, send_dy = dispatch(
        block_expert,
        block_count,
        new_owner,
        tokens.reshape(blocks, rows, features),
        cotangent.reshape(blocks, rows, features),
    )
    send_x, _ = lax.optimization_barrier((send_x, down_pair))
    inputs = exchange(send_x, "expert")
    send_dy, inputs = lax.optimization_barrier((send_dy, inputs))
    inputs = inputs.reshape(-1, features)
    upstream = exchange(send_dy, "expert").reshape(-1, features)
    inputs_other, upstream_other = from_partner(inputs), from_partner(upstream)

    packed = pack_states(
        (up_first[0], up_second[0]), (down_first[0], down_second[0]), groups
    )
    packed, upstream = lax.optimization_barrier((packed, upstream))
    shares = exchange(packed, "expert")

    pre_act = jnp.dot(inputs, up_mat, preferred_element_type=F32)
    active, slopes = silu_parts(pre_act)
    hidden = active.astype(BF)
    hidden_other = from_partner(hidden)
    down_part = weight_grad(down_place, hidden, hidden_other, upstream, upstream_other, 128)
    tall = down_shape[0]
    rising = [(i, (i + 1) % NY) for i in range(NY)]
    falling = [(i, (i - 1) % NY) for i in range(NY)]
    below = lax.ppermute(down_part[4 * tall : 5 * tall], "y", rising)
    above = lax.ppermute(down_part[5 * tall : 6 * tall], "y", falling)
    upstream, _ = lax.optimization_barrier((upstream, down_part))
    back = lax.dot_general(upstream, down_mat, (((1,), (1,)), ((), ())), preferred_element_type=F32)
    pre_grad = (back * slopes).astype(BF)
    pre_grad_other = from_partner(pre_grad)
    up_part = weight_grad(up_place, inputs, inputs_other, pre_grad, pre_grad_other, 256)
    up_grad = lax.psum_scatter(up_part, ("y", "x"), scatter_dimension=0, tiled=True)
    pre_grad, up_part = lax.optimization_barrier((pre_grad, up_part))
    going_up, going_down = relay(down_part, below, above)
    below = lax.ppermute(going_up, "y", rising)
    above = lax.ppermute(going_down, "y", falling)
    input_grad = lax.dot_general(
        pre_grad, up_mat, (((1,), (1,)), ((), ())), preferred_element_type=F32
    ).astype(BF)
    input_grad, shares = lax.optimization_barrier((input_grad, shares))
    returned = exchange(input_grad.reshape(-1, rows, features), "expert")
    ordered = order_states(old_owner, new_owner, shares, 1)
    ordered, returned = lax.optimization_barrier((ordered, returned))
    states = exchange(ordered, "expert")
    token_grad = combine(block_expert, new_owner, returned).reshape(tok_rows, features)

    down_own, down_send = finish(x_at, down_part, below, above)
    down_other = lax.ppermute(down_send, "x", [(0, 1), (1, 0)])
    down_new = adam(
        adam_down_body, x_at, down_shares, states, 1, (down_own, down_other), down_shape,
    )
    up_new = adam(adam_up_body, x_at, up_shares, states, 0, (up_grad,), up_shape)
    return (
        token_grad,
        up_new[0][None],
        down_new[0][None],
        up_new[1][None],
        up_new[2][None],
        down_new[1][None],
        down_new[2][None],
    )


def solution(mesh):
    fine = Mesh(
        mesh.devices.reshape(mesh.devices.shape[0], NX, NY, NC), ("expert", "x", "y", "core")
    )
    every = ("expert", "x", "y", "core")
    dp = ("x", "y", "core")
    state = P("expert", dp, None)
    return jax.shard_map(
        step,
        mesh=fine,
        in_specs=(P(every, None), P(every, None), P(every, None), P(every), P(), P())
        + (state,) * 6,
        out_specs=(P(every, None),) + (state,) * 6,
        check_vma=False,
    )
```

```python
import jax
import jax.numpy as jnp
from jax import lax
from jax.experimental import pallas as pl
from jax.experimental.pallas import tpu as pltpu
from jax.sharding import Mesh
from jax.sharding import PartitionSpec as P


beta_one = 0.9
beta_two = 0.95
bias_one = 1.0 - 0.9**10
bias_two = 1.0 - 0.95**10
rate_value = 0.01
decay_value = 0.1
eps_value = 1e-08

F32 = jnp.float32
BF = jnp.bfloat16
NX, NY, NC = 2, 4, 2
LANE = 128


def row_order():
    return [x * NY * NC + y * NC + c for c in range(NC) for y in range(NY) for x in range(NX)]


def inverse(order):
    back = [0] * len(order)
    for p, r in enumerate(order):
        back[r] = p
    return back


def lanes_taken(value, order):
    width = value.shape[1] // len(order)
    return jnp.concatenate([value[:, r * width : (r + 1) * width] for r in order], axis=1)


def pack_weights_body(up_ref, down_ref, out_ref):
    for g in range(out_ref.shape[0]):
        out_ref[g, 0] = up_ref[:, g * LANE : (g + 1) * LANE].astype(BF)
        out_ref[g, 1] = to_tiles(down_ref[g * 8 : (g + 1) * 8]).astype(BF)


def pack_weights(up, down, groups):
    return pl.pallas_call(
        pack_weights_body,
        out_shape=jax.ShapeDtypeStruct((groups, 2, up.shape[0], LANE), BF),
        name="pack_weights",
    )(up, down)


def unpack_body(in_ref, up_ref, down_ref):
    groups = in_ref.shape[0] // NX
    rows, tall = up_ref.shape[0] // NX, down_ref.shape[0] // NX
    for x in range(NX):
        shares = [in_ref[g * NX + x].astype(F32) for g in range(groups)]
        up = jnp.concatenate([share[0] for share in shares], axis=1)
        up_ref[x * rows : (x + 1) * rows] = lanes_taken(up, row_order()).astype(BF)
        down = jnp.concatenate([from_tiles(share[1]) for share in shares], axis=0)
        down_ref[x * tall : (x + 1) * tall] = down.astype(BF)


def unpack_weights(shares, up_shape, down_shape):
    return pl.pallas_call(
        unpack_body,
        out_shape=(
            jax.ShapeDtypeStruct((NX * up_shape[0], up_shape[1]), BF),
            jax.ShapeDtypeStruct((NX * down_shape[0], down_shape[1]), BF),
        ),
        name="unpack_weights",
    )(shares)


def slot_of_block(ids_ref, own_ref, b):
    mine = ids_ref[b, 0]
    place = jnp.int32(0)
    for e in range(b):
        place = place + (ids_ref[e, 0] == mine).astype(jnp.int32)
    return own_ref[mine] * 2 + place


def dispatch_body(ids_ref, count_ref, own_ref, tok_ref, cot_ref, sx_ref, sdy_ref):
    blocks, rows, _ = tok_ref.shape
    sx_ref[...] = jnp.zeros(sx_ref.shape, BF)
    sdy_ref[...] = jnp.zeros(sdy_ref.shape, BF)
    at = lax.broadcasted_iota(jnp.int32, (rows, 1), 0)
    for b in range(blocks):
        slot = slot_of_block(ids_ref, own_ref, b)
        alive = at < count_ref[b]
        x = jnp.where(alive, tok_ref[b].astype(F32), 0.0)
        dy = jnp.where(alive, cot_ref[b].astype(F32), 0.0)
        sx_ref[slot] = lanes_taken(x, row_order()).astype(BF)
        sdy_ref[slot] = dy.astype(BF)


def smem():
    return pl.BlockSpec(memory_space=pltpu.SMEM)


def vmem():
    return pl.BlockSpec(memory_space=pltpu.VMEM)


def dispatch(ids, count, owner, tokens, cotangent):
    blocks, rows, width = tokens.shape
    out = jax.ShapeDtypeStruct((2 * blocks, rows, width), BF)
    return pl.pallas_call(
        dispatch_body,
        in_specs=[smem(), smem(), smem(), vmem(), vmem()],
        out_shape=(out, out),
        name="dispatch",
    )(ids, count, owner, tokens, cotangent)


def combine_body(ids_ref, own_ref, ret_ref, out_ref):
    for b in range(out_ref.shape[0]):
        slot = slot_of_block(ids_ref, own_ref, b)
        out_ref[b] = lanes_taken(ret_ref[slot].astype(F32), inverse(row_order())).astype(BF)


def combine(ids, owner, returned):
    slots, rows, width = returned.shape
    return pl.pallas_call(
        combine_body,
        in_specs=[smem(), smem(), vmem()],
        out_shape=jax.ShapeDtypeStruct((slots // 2, rows, width), BF),
        name="combine",
    )(ids, owner, returned)


def to_tiles(rows8):
    n = rows8.shape[1] // LANE
    return jnp.concatenate([rows8[:, i * LANE : (i + 1) * LANE] for i in range(n)], axis=0)


def from_tiles(tiles):
    n = tiles.shape[0] // 8
    return jnp.concatenate([tiles[i * 8 : (i + 1) * 8] for i in range(n)], axis=1)


def pack_body(a_ref, b_ref, c_ref, d_ref, out_ref):
    for g in range(out_ref.shape[0]):
        for i, ref in enumerate((a_ref, b_ref)):
            out_ref[g, i] = ref[:, g * LANE : (g + 1) * LANE].astype(BF)
        for i, ref in enumerate((c_ref, d_ref)):
            out_ref[g, 2 + i] = to_tiles(ref[g * 8 : (g + 1) * 8]).astype(BF)


def pack_states(ups, downs, groups):
    rows, cols = ups[0].shape
    return pl.pallas_call(
        pack_body,
        out_shape=jax.ShapeDtypeStruct((groups, 4, rows, cols // groups), BF),
        name="pack_states",
    )(*ups, *downs)


def order_body(old_ref, new_ref, in_ref, out_ref):
    copies = out_ref.shape[0] // in_ref.shape[0]
    for k in range(in_ref.shape[0]):
        for i in range(copies):
            out_ref[new_ref[k] * copies + i] = in_ref[old_ref[k]]


def order_states(old, new, shares, copies):
    shape = (shares.shape[0] * copies,) + shares.shape[1:]
    return pl.pallas_call(
        order_body, in_specs=[smem(), smem(), vmem()], out_shape=jax.ShapeDtypeStruct(shape, BF)
    )(old, new, shares)


def weight_grad_body(half_ref, a_ref, ao_ref, b_ref, bo_ref, out_ref):
    dims = (((0,), (0,)), ((), ()))
    total = lax.dot_general(a_ref[...], b_ref[...], dims, preferred_element_type=F32)
    total += lax.dot_general(ao_ref[...], bo_ref[...], dims, preferred_element_type=F32)
    out_ref[...] = total.astype(BF)


def weight_grad(place, a, a_other, b, b_other, step):
    rows, width = a.shape
    cols = b.shape[1]
    steps = width // 2 // step
    left = pl.BlockSpec(
        (rows, step), lambda i, at: (0, at[0] * steps + lax.rem(at[1] + i, steps))
    )
    right = pl.BlockSpec((rows, cols), lambda i, at: (0, 0))
    return pl.pallas_call(
        weight_grad_body,
        grid_spec=pltpu.PrefetchScalarGridSpec(
            num_scalar_prefetch=1,
            grid=(steps,),
            in_specs=[left, left, right, right],
            out_specs=pl.BlockSpec((step, cols), lambda i, at: (i, 0)),
        ),
        out_shape=jax.ShapeDtypeStruct((width // 2, cols), BF),
    )(place, a, a_other, b, b_other)


def relay_body(part_ref, below_ref, above_ref, up_ref, down_ref):
    tall = below_ref.shape[0]
    wide = 2 * tall
    mine = part_ref[wide : 2 * wide].astype(F32)
    up_ref[0:tall] = (mine[0:tall] + below_ref[...].astype(F32)).astype(BF)
    up_ref[tall:wide] = part_ref[wide + tall : 2 * wide]
    mine = part_ref[3 * wide + tall : 4 * wide].astype(F32)
    down_ref[0:tall] = part_ref[3 * wide : 3 * wide + tall]
    down_ref[tall:wide] = (mine + above_ref[...].astype(F32)).astype(BF)


def relay(part, below, above):
    tall, cols = below.shape
    out = jax.ShapeDtypeStruct((2 * tall, cols), BF)
    return pl.pallas_call(relay_body, out_shape=(out, out), name="relay")(part, below, above)


def finish_body(x_ref, part_ref, below_ref, above_ref, own_ref, send_ref):
    tall = own_ref.shape[0]
    total = part_ref[...].astype(F32) + below_ref[...].astype(F32) + above_ref[...].astype(F32)
    low, high = total[0:tall], total[tall : 2 * tall]
    first = x_ref[0] == 0
    own_ref[...] = jnp.where(first, low, high)
    send_ref[...] = jnp.where(first, high, low).astype(BF)


def finish(x_at, part, below, above):
    wide, cols = below.shape
    whole = pl.BlockSpec((wide, cols), lambda i: (0, 0))
    half_spec = pl.BlockSpec((wide // 2, cols), lambda i: (0, 0))
    return pl.pallas_call(
        finish_body,
        grid=(1,),
        in_specs=[smem(), whole, whole, whole],
        out_specs=(half_spec, half_spec),
        out_shape=(
            jax.ShapeDtypeStruct((wide // 2, cols), F32),
            jax.ShapeDtypeStruct((wide // 2, cols), BF),
        ),
        name="finish",
    )(x_at, part, below, above)


def adam_update(weight, moment, second, gradient):
    moment_new = beta_one * moment + (1.0 - beta_one) * gradient
    second_new = beta_two * second + (1.0 - beta_two) * gradient * gradient
    update = moment_new / bias_one / (jnp.sqrt(second_new / bias_two) + eps_value)
    return (weight - rate_value * (update + decay_value * weight), moment_new, second_new)


def adam_up_body(x_ref, weight_ref, state_ref, grad_ref, other_ref, *outs):
    rows = other_ref.shape[0]
    own = grad_ref[pl.ds(pl.multiple_of(x_ref[0] * rows, 16), rows)]
    both = own.astype(F32) + other_ref[...].astype(F32)
    grad = lanes_taken(both, inverse(row_order()))
    for g in range(state_ref.shape[0]):
        lanes = slice(g * LANE, (g + 1) * LANE)
        m, v = (state_ref[g, i].astype(F32) for i in range(2))
        w = weight_ref[g * NX + x_ref[0], 0].astype(F32)
        for ref, value in zip(outs, adam_update(w, m, v, grad[:, lanes])):
            ref[:, lanes] = value


def adam_down_body(x_ref, weight_ref, state_ref, grad_ref, other_ref, *outs):
    for g in range(state_ref.shape[0]):
        rows = slice(g * 8, (g + 1) * 8)
        m, v = (from_tiles(state_ref[g, i].astype(F32)) for i in range(2))
        w = from_tiles(weight_ref[g * NX + x_ref[0], 0].astype(F32))
        grad = grad_ref[rows] + other_ref[rows].astype(F32)
        for ref, value in zip(outs, adam_update(w, m, v, grad)):
            ref[rows] = value


def adam(body, x_at, weights, states, which, grads, shape):
    groups, _, rows, wide = states.shape
    full = pl.BlockSpec(shape, lambda i: (0, 0))
    return pl.pallas_call(
        body,
        grid=(1,),
        in_specs=[
            smem(),
            pl.BlockSpec((weights.shape[0], 1, rows, wide), lambda i: (0, which, 0, 0)),
            pl.BlockSpec((groups, 2, rows, wide), lambda i: (0, which, 0, 0)),
        ]
        + [pl.BlockSpec(g.shape, lambda i: (0, 0)) for g in grads],
        out_specs=[full] * 3,
        out_shape=[jax.ShapeDtypeStruct(shape, F32)] * 3,
    )(x_at, weights, states, *grads)


def silu_parts(pre_act):
    sigma = jax.nn.sigmoid(pre_act)
    return (pre_act * sigma, sigma * (1.0 + pre_act * (1.0 - sigma)))


def exchange(array, axis):
    return lax.all_to_all(array, axis, split_axis=0, concat_axis=0, tiled=True)


def from_partner(array):
    return lax.ppermute(array, "core", [(0, 1), (1, 0)])


def step(
    tokens,
    cotangent,
    block_expert,
    block_count,
    old_owner,
    new_owner,
    up_weight,
    down_weight,
    up_first,
    up_second,
    down_first,
    down_second,
):
    groups = lax.axis_size("expert")
    tok_rows, features = tokens.shape
    blocks = block_count.shape[0]
    rows = tok_rows // blocks
    core_at = lax.axis_index("core").astype(jnp.int32)
    y_at = lax.axis_index("y").astype(jnp.int32)
    x_at = lax.axis_index("x").astype(jnp.int32).reshape(1)
    up_place = jnp.stack([core_at, jnp.zeros((), jnp.int32)])
    down_place = jnp.stack([core_at, y_at])
    up_shape, down_shape = up_weight.shape[1:], down_weight.shape[1:]

    packed = pack_weights(up_weight[0], down_weight[0], groups)
    spread = exchange(packed, "expert")
    ordered = order_states(old_owner, new_owner, spread, NX)
    weights = exchange(ordered, ("expert", "x"))
    up_pair, down_pair = unpack_weights(weights, up_shape, down_shape)
    up_mat = lax.all_gather(up_pair, ("core", "y"), axis=0, tiled=True)
    down_mat = lax.all_gather(down_pair, ("core", "y"), axis=0, tiled=True)

    send_x, send_dy = dispatch(
        block_expert,
        block_count,
        new_owner,
        tokens.reshape(blocks, rows, features),
        cotangent.reshape(blocks, rows, features),
    )
    send_x, _ = lax.optimization_barrier((send_x, down_pair))
    inputs = exchange(send_x, "expert")
    send_dy, inputs = lax.optimization_barrier((send_dy, inputs))
    inputs = inputs.reshape(-1, features)
    upstream = exchange(send_dy, "expert").reshape(-1, features)
    inputs_other, upstream_other = from_partner(inputs), from_partner(upstream)

    packed = pack_states(
        (up_first[0], up_second[0]), (down_first[0], down_second[0]), groups
    )
    packed, upstream = lax.optimization_barrier((packed, upstream))
    shares = exchange(packed, "expert")

    pre_act = jnp.dot(inputs, up_mat, preferred_element_type=F32)
    active, slopes = silu_parts(pre_act)
    hidden = active.astype(BF)
    hidden_other = from_partner(hidden)
    down_part = weight_grad(down_place, hidden, hidden_other, upstream, upstream_other, 128)
    tall = down_shape[0]
    rising = [(i, (i + 1) % NY) for i in range(NY)]
    falling = [(i, (i - 1) % NY) for i in range(NY)]
    below = lax.ppermute(down_part[4 * tall : 5 * tall], "y", rising)
    above = lax.ppermute(down_part[5 * tall : 6 * tall], "y", falling)
    going_up, going_down = relay(down_part, below, above)
    below = lax.ppermute(going_up, "y", rising)
    above = lax.ppermute(going_down, "y", falling)
    ordered = order_states(old_owner, new_owner, shares, 1)
    states = exchange(ordered, "expert")
    back = lax.dot_general(upstream, down_mat, (((1,), (1,)), ((), ())), preferred_element_type=F32)
    pre_grad = (back * slopes).astype(BF)
    pre_grad_other = from_partner(pre_grad)
    up_part = weight_grad(up_place, inputs, inputs_other, pre_grad, pre_grad_other, 256)
    up_sum = lax.psum_scatter(up_part, "y", scatter_dimension=0, tiled=True)
    pre_grad, up_part = lax.optimization_barrier((pre_grad, up_part))
    input_grad = lax.dot_general(
        pre_grad, up_mat, (((1,), (1,)), ((), ())), preferred_element_type=F32
    ).astype(BF)
    input_grad, states = lax.optimization_barrier((input_grad, states))
    returned = exchange(input_grad.reshape(-1, rows, features), "expert")
    token_grad = combine(block_expert, new_owner, returned).reshape(tok_rows, features)

    swap = [(0, 1), (1, 0)]
    down_own, down_send = finish(x_at, down_part, below, above)
    down_other = lax.ppermute(down_send, "x", swap)
    up_send = lax.dynamic_slice_in_dim(up_sum, (1 - x_at[0]) * up_shape[0], up_shape[0])
    up_other = lax.ppermute(up_send, "x", swap)
    down_new = adam(adam_down_body, x_at, weights, states, 1, (down_own, down_other), down_shape)
    up_new = adam(adam_up_body, x_at, weights, states, 0, (up_sum, up_other), up_shape)
    return (
        token_grad,
        up_new[0][None],
        down_new[0][None],
        up_new[1][None],
        up_new[2][None],
        down_new[1][None],
        down_new[2][None],
    )


def solution(mesh):
    fine = Mesh(
        mesh.devices.reshape(mesh.devices.shape[0], NX, NY, NC), ("expert", "x", "y", "core")
    )
    every = ("expert", "x", "y", "core")
    dp = ("x", "y", "core")
    state = P("expert", dp, None)
    return jax.shard_map(
        step,
        mesh=fine,
        in_specs=(P(every, None), P(every, None), P(every, None), P(every), P(), P())
        + (state,) * 6,
        out_specs=(P(every, None),) + (state,) * 6,
        check_vma=False,
    )
```

```python
import jax
import jax.numpy as jnp
from jax import lax
from jax.experimental import pallas as pl
from jax.experimental.pallas import tpu as pltpu
from jax.sharding import Mesh
from jax.sharding import PartitionSpec as P


beta_one = 0.9
beta_two = 0.95
bias_one = 1.0 - 0.9**10
bias_two = 1.0 - 0.95**10
rate_value = 0.01
decay_value = 0.1
eps_value = 1e-08

F32 = jnp.float32
BF = jnp.bfloat16
NX, NY, NC = 2, 4, 2
LANE = 128


def row_order():
    return [x * NY * NC + y * NC + c for c in range(NC) for y in range(NY) for x in range(NX)]


def inverse(order):
    back = [0] * len(order)
    for p, r in enumerate(order):
        back[r] = p
    return back


def lanes_taken(value, order):
    width = value.shape[1] // len(order)
    return jnp.concatenate([value[:, r * width : (r + 1) * width] for r in order], axis=1)


def pack_weights_body(up_ref, down_ref, out_ref):
    for g in range(out_ref.shape[0]):
        out_ref[g, 0] = up_ref[:, g * LANE : (g + 1) * LANE].astype(BF)
        out_ref[g, 1] = to_tiles(down_ref[g * 8 : (g + 1) * 8]).astype(BF)


def pack_weights(up, down, groups):
    return pl.pallas_call(
        pack_weights_body,
        out_shape=jax.ShapeDtypeStruct((groups, 2, up.shape[0], LANE), BF),
        name="pack_weights",
    )(up, down)


def unpack_body(in_ref, up_ref, down_ref):
    groups = in_ref.shape[0] // NX
    rows, tall = up_ref.shape[0] // NX, down_ref.shape[0] // NX
    for x in range(NX):
        shares = [in_ref[g * NX + x].astype(F32) for g in range(groups)]
        up = jnp.concatenate([share[0] for share in shares], axis=1)
        up_ref[x * rows : (x + 1) * rows] = lanes_taken(up, row_order()).astype(BF)
        down = jnp.concatenate([from_tiles(share[1]) for share in shares], axis=0)
        down_ref[x * tall : (x + 1) * tall] = down.astype(BF)


def unpack_weights(shares, up_shape, down_shape):
    return pl.pallas_call(
        unpack_body,
        out_shape=(
            jax.ShapeDtypeStruct((NX * up_shape[0], up_shape[1]), BF),
            jax.ShapeDtypeStruct((NX * down_shape[0], down_shape[1]), BF),
        ),
        name="unpack_weights",
    )(shares)


def slot_of_block(ids_ref, own_ref, b):
    mine = ids_ref[b, 0]
    place = jnp.int32(0)
    for e in range(b):
        place = place + (ids_ref[e, 0] == mine).astype(jnp.int32)
    return own_ref[mine] * 2 + place


def dispatch_body(ids_ref, count_ref, own_ref, tok_ref, cot_ref, sx_ref, sdy_ref):
    blocks, rows, _ = tok_ref.shape
    sx_ref[...] = jnp.zeros(sx_ref.shape, BF)
    sdy_ref[...] = jnp.zeros(sdy_ref.shape, BF)
    at = lax.broadcasted_iota(jnp.int32, (rows, 1), 0)
    for b in range(blocks):
        slot = slot_of_block(ids_ref, own_ref, b)
        alive = at < count_ref[b]
        x = jnp.where(alive, tok_ref[b].astype(F32), 0.0)
        dy = jnp.where(alive, cot_ref[b].astype(F32), 0.0)
        sx_ref[slot] = lanes_taken(x, row_order()).astype(BF)
        sdy_ref[slot] = dy.astype(BF)


def smem():
    return pl.BlockSpec(memory_space=pltpu.SMEM)


def vmem():
    return pl.BlockSpec(memory_space=pltpu.VMEM)


def dispatch(ids, count, owner, tokens, cotangent):
    blocks, rows, width = tokens.shape
    out = jax.ShapeDtypeStruct((2 * blocks, rows, width), BF)
    return pl.pallas_call(
        dispatch_body,
        in_specs=[smem(), smem(), smem(), vmem(), vmem()],
        out_shape=(out, out),
        name="dispatch",
    )(ids, count, owner, tokens, cotangent)


def combine_body(ids_ref, own_ref, ret_ref, out_ref):
    for b in range(out_ref.shape[0]):
        slot = slot_of_block(ids_ref, own_ref, b)
        out_ref[b] = lanes_taken(ret_ref[slot].astype(F32), inverse(row_order())).astype(BF)


def combine(ids, owner, returned):
    slots, rows, width = returned.shape
    return pl.pallas_call(
        combine_body,
        in_specs=[smem(), smem(), vmem()],
        out_shape=jax.ShapeDtypeStruct((slots // 2, rows, width), BF),
        name="combine",
    )(ids, owner, returned)


def to_tiles(rows8):
    n = rows8.shape[1] // LANE
    return jnp.concatenate([rows8[:, i * LANE : (i + 1) * LANE] for i in range(n)], axis=0)


def from_tiles(tiles):
    n = tiles.shape[0] // 8
    return jnp.concatenate([tiles[i * 8 : (i + 1) * 8] for i in range(n)], axis=1)


def pack_body(a_ref, b_ref, c_ref, d_ref, out_ref):
    for g in range(out_ref.shape[0]):
        for i, ref in enumerate((a_ref, b_ref)):
            out_ref[g, i] = ref[:, g * LANE : (g + 1) * LANE].astype(BF)
        for i, ref in enumerate((c_ref, d_ref)):
            out_ref[g, 2 + i] = to_tiles(ref[g * 8 : (g + 1) * 8]).astype(BF)


def pack_states(ups, downs, groups):
    rows, cols = ups[0].shape
    return pl.pallas_call(
        pack_body,
        out_shape=jax.ShapeDtypeStruct((groups, 4, rows, cols // groups), BF),
        name="pack_states",
    )(*ups, *downs)


def order_body(old_ref, new_ref, in_ref, out_ref):
    copies = out_ref.shape[0] // in_ref.shape[0]
    for k in range(in_ref.shape[0]):
        for i in range(copies):
            out_ref[new_ref[k] * copies + i] = in_ref[old_ref[k]]


def order_states(old, new, shares, copies):
    shape = (shares.shape[0] * copies,) + shares.shape[1:]
    return pl.pallas_call(
        order_body, in_specs=[smem(), smem(), vmem()], out_shape=jax.ShapeDtypeStruct(shape, BF)
    )(old, new, shares)


def weight_grad_body(half_ref, a_ref, ao_ref, b_ref, bo_ref, out_ref):
    dims = (((0,), (0,)), ((), ()))
    total = lax.dot_general(a_ref[...], b_ref[...], dims, preferred_element_type=F32)
    total += lax.dot_general(ao_ref[...], bo_ref[...], dims, preferred_element_type=F32)
    out_ref[...] = total.astype(BF)


def weight_grad(place, a, a_other, b, b_other, step):
    rows, width = a.shape
    cols = b.shape[1]
    steps = width // 2 // step
    left = pl.BlockSpec(
        (rows, step), lambda i, at: (0, at[0] * steps + lax.rem(at[1] + i, steps))
    )
    right = pl.BlockSpec((rows, cols), lambda i, at: (0, 0))
    return pl.pallas_call(
        weight_grad_body,
        grid_spec=pltpu.PrefetchScalarGridSpec(
            num_scalar_prefetch=1,
            grid=(steps,),
            in_specs=[left, left, right, right],
            out_specs=pl.BlockSpec((step, cols), lambda i, at: (i, 0)),
        ),
        out_shape=jax.ShapeDtypeStruct((width // 2, cols), BF),
    )(place, a, a_other, b, b_other)


def flip_body(core_ref, own_ref, other_ref, out_ref):
    rows = own_ref.shape[0]
    out_ref[:, 0:rows] = own_ref[...].astype(F32).T.astype(BF)
    out_ref[:, rows : 2 * rows] = other_ref[...].astype(F32).T.astype(BF)


def flip(place, own, other, step=256):
    rows, width = own.shape
    steps = width // 2 // step
    part = pl.BlockSpec((rows, step), lambda i, at: (0, at[0] * steps + i))
    return pl.pallas_call(
        flip_body,
        grid_spec=pltpu.PrefetchScalarGridSpec(
            num_scalar_prefetch=1,
            grid=(steps,),
            in_specs=[part, part],
            out_specs=pl.BlockSpec((step, 2 * rows), lambda i, at: (i, 0)),
        ),
        out_shape=jax.ShapeDtypeStruct((width // 2, 2 * rows), BF),
        name="flip",
    )(place, own, other)


def half_grad_body(at_ref, xt_ref, own_ref, other_ref, out_ref):
    rows = own_ref.shape[0]
    total = jnp.dot(xt_ref[:, 0:rows], own_ref[...], preferred_element_type=F32)
    total += jnp.dot(xt_ref[:, rows : 2 * rows], other_ref[...], preferred_element_type=F32)
    out_ref[...] = total.astype(BF)


def half_grad(which, flipped, own, other):
    width, deep = flipped.shape
    rows, cols = own.shape
    tall = width // (NX * NY)
    right = pl.BlockSpec((rows, cols), lambda i, at: (0, 0))
    return pl.pallas_call(
        half_grad_body,
        grid_spec=pltpu.PrefetchScalarGridSpec(
            num_scalar_prefetch=1,
            grid=(NY,),
            in_specs=[pl.BlockSpec((tall, deep), lambda i, at: (i * NX + at[0], 0)), right, right],
            out_specs=pl.BlockSpec((tall, cols), lambda i, at: (i, 0)),
        ),
        out_shape=jax.ShapeDtypeStruct((width // NX, cols), BF),
    )(which, flipped, own, other)


def relay_body(part_ref, below_ref, above_ref, up_ref, down_ref):
    tall = below_ref.shape[0]
    wide = 2 * tall
    mine = part_ref[wide : 2 * wide].astype(F32)
    up_ref[0:tall] = (mine[0:tall] + below_ref[...].astype(F32)).astype(BF)
    up_ref[tall:wide] = part_ref[wide + tall : 2 * wide]
    mine = part_ref[3 * wide + tall : 4 * wide].astype(F32)
    down_ref[0:tall] = part_ref[3 * wide : 3 * wide + tall]
    down_ref[tall:wide] = (mine + above_ref[...].astype(F32)).astype(BF)


def relay(part, below, above):
    tall, cols = below.shape
    out = jax.ShapeDtypeStruct((2 * tall, cols), BF)
    return pl.pallas_call(relay_body, out_shape=(out, out), name="relay")(part, below, above)


def finish_body(x_ref, part_ref, below_ref, above_ref, own_ref, send_ref):
    tall = own_ref.shape[0]
    total = part_ref[...].astype(F32) + below_ref[...].astype(F32) + above_ref[...].astype(F32)
    low, high = total[0:tall], total[tall : 2 * tall]
    first = x_ref[0] == 0
    own_ref[...] = jnp.where(first, low, high)
    send_ref[...] = jnp.where(first, high, low).astype(BF)


def finish(x_at, part, below, above):
    wide, cols = below.shape
    whole = pl.BlockSpec((wide, cols), lambda i: (0, 0))
    half_spec = pl.BlockSpec((wide // 2, cols), lambda i: (0, 0))
    return pl.pallas_call(
        finish_body,
        grid=(1,),
        in_specs=[smem(), whole, whole, whole],
        out_specs=(half_spec, half_spec),
        out_shape=(
            jax.ShapeDtypeStruct((wide // 2, cols), F32),
            jax.ShapeDtypeStruct((wide // 2, cols), BF),
        ),
        name="finish",
    )(x_at, part, below, above)


def adam_update(weight, moment, second, gradient):
    moment_new = beta_one * moment + (1.0 - beta_one) * gradient
    second_new = beta_two * second + (1.0 - beta_two) * gradient * gradient
    update = moment_new / bias_one / (jnp.sqrt(second_new / bias_two) + eps_value)
    return (weight - rate_value * (update + decay_value * weight), moment_new, second_new)


def adam_up_body(x_ref, weight_ref, state_ref, grad_ref, other_ref, *outs):
    both = grad_ref[...].astype(F32) + other_ref[...].astype(F32)
    grad = lanes_taken(both, inverse(row_order()))
    for g in range(state_ref.shape[0]):
        lanes = slice(g * LANE, (g + 1) * LANE)
        m, v = (state_ref[g, i].astype(F32) for i in range(2))
        w = weight_ref[g * NX + x_ref[0], 0].astype(F32)
        for ref, value in zip(outs, adam_update(w, m, v, grad[:, lanes])):
            ref[:, lanes] = value


def adam_down_body(x_ref, weight_ref, state_ref, grad_ref, other_ref, *outs):
    for g in range(state_ref.shape[0]):
        rows = slice(g * 8, (g + 1) * 8)
        m, v = (from_tiles(state_ref[g, i].astype(F32)) for i in range(2))
        w = from_tiles(weight_ref[g * NX + x_ref[0], 0].astype(F32))
        grad = grad_ref[rows] + other_ref[rows].astype(F32)
        for ref, value in zip(outs, adam_update(w, m, v, grad)):
            ref[rows] = value


def adam(body, x_at, weights, states, which, grads, shape):
    groups, _, rows, wide = states.shape
    full = pl.BlockSpec(shape, lambda i: (0, 0))
    return pl.pallas_call(
        body,
        grid=(1,),
        in_specs=[
            smem(),
            pl.BlockSpec((weights.shape[0], 1, rows, wide), lambda i: (0, which, 0, 0)),
            pl.BlockSpec((groups, 2, rows, wide), lambda i: (0, which, 0, 0)),
        ]
        + [pl.BlockSpec(g.shape, lambda i: (0, 0)) for g in grads],
        out_specs=[full] * 3,
        out_shape=[jax.ShapeDtypeStruct(shape, F32)] * 3,
    )(x_at, weights, states, *grads)


def silu_parts(pre_act):
    sigma = jax.nn.sigmoid(pre_act)
    return (pre_act * sigma, sigma * (1.0 + pre_act * (1.0 - sigma)))


def exchange(array, axis):
    return lax.all_to_all(array, axis, split_axis=0, concat_axis=0, tiled=True)


def from_partner(array):
    return lax.ppermute(array, "core", [(0, 1), (1, 0)])


def step(
    tokens,
    cotangent,
    block_expert,
    block_count,
    old_owner,
    new_owner,
    up_weight,
    down_weight,
    up_first,
    up_second,
    down_first,
    down_second,
):
    groups = lax.axis_size("expert")
    tok_rows, features = tokens.shape
    blocks = block_count.shape[0]
    rows = tok_rows // blocks
    core_at = lax.axis_index("core").astype(jnp.int32)
    y_at = lax.axis_index("y").astype(jnp.int32)
    x_at = lax.axis_index("x").astype(jnp.int32).reshape(1)
    down_place = jnp.stack([core_at, y_at])
    up_shape, down_shape = up_weight.shape[1:], down_weight.shape[1:]

    packed = pack_weights(up_weight[0], down_weight[0], groups)
    spread = exchange(packed, "expert")
    ordered = order_states(old_owner, new_owner, spread, NX)
    weights = exchange(ordered, ("expert", "x"))
    up_pair, down_pair = unpack_weights(weights, up_shape, down_shape)
    up_mat = lax.all_gather(up_pair, ("core", "y"), axis=0, tiled=True)
    down_mat = lax.all_gather(down_pair, ("core", "y"), axis=0, tiled=True)

    send_x, send_dy = dispatch(
        block_expert,
        block_count,
        new_owner,
        tokens.reshape(blocks, rows, features),
        cotangent.reshape(blocks, rows, features),
    )
    send_x, _ = lax.optimization_barrier((send_x, down_pair))
    inputs = exchange(send_x, "expert")
    send_dy, inputs = lax.optimization_barrier((send_dy, inputs))
    inputs = inputs.reshape(-1, features)
    upstream = exchange(send_dy, "expert").reshape(-1, features)
    inputs_other, upstream_other = from_partner(inputs), from_partner(upstream)

    packed = pack_states(
        (up_first[0], up_second[0]), (down_first[0], down_second[0]), groups
    )
    packed, upstream = lax.optimization_barrier((packed, upstream))
    shares = exchange(packed, "expert")

    pre_act = jnp.dot(inputs, up_mat, preferred_element_type=F32)
    active, slopes = silu_parts(pre_act)
    hidden = active.astype(BF)
    hidden_other = from_partner(hidden)
    down_part = weight_grad(down_place, hidden, hidden_other, upstream, upstream_other, 128)
    tall = down_shape[0]
    rising = [(i, (i + 1) % NY) for i in range(NY)]
    falling = [(i, (i - 1) % NY) for i in range(NY)]
    below = lax.ppermute(down_part[4 * tall : 5 * tall], "y", rising)
    above = lax.ppermute(down_part[5 * tall : 6 * tall], "y", falling)
    flipped = flip(down_place, inputs, inputs_other)
    upstream, flipped, _ = lax.optimization_barrier((upstream, flipped, down_part))
    back = lax.dot_general(upstream, down_mat, (((1,), (1,)), ((), ())), preferred_element_type=F32)
    pre_grad = (back * slopes).astype(BF)
    pre_grad_other = from_partner(pre_grad)
    ordered = order_states(old_owner, new_owner, shares, 1)
    ordered, pre_grad = lax.optimization_barrier((ordered, pre_grad))
    states = exchange(ordered, "expert")
    up_far = half_grad(1 - x_at, flipped, pre_grad, pre_grad_other)
    up_far_sum = lax.psum_scatter(up_far, "y", scatter_dimension=0, tiled=True)
    pre_grad, up_far = lax.optimization_barrier((pre_grad, up_far))
    up_own = half_grad(x_at, flipped, pre_grad, pre_grad_other)
    up_sum = lax.psum_scatter(up_own, "y", scatter_dimension=0, tiled=True)
    pre_grad, down_part, up_own = lax.optimization_barrier((pre_grad, down_part, up_own))
    going_up, going_down = relay(down_part, below, above)
    below = lax.ppermute(going_up, "y", rising)
    above = lax.ppermute(going_down, "y", falling)
    input_grad = lax.dot_general(
        pre_grad, up_mat, (((1,), (1,)), ((), ())), preferred_element_type=F32
    ).astype(BF)
    input_grad, states = lax.optimization_barrier((input_grad, states))
    returned = exchange(input_grad.reshape(-1, rows, features), "expert")
    token_grad = combine(block_expert, new_owner, returned).reshape(tok_rows, features)

    swap = [(0, 1), (1, 0)]
    down_own, down_send = finish(x_at, down_part, below, above)
    down_other = lax.ppermute(down_send, "x", swap)
    up_other = lax.ppermute(up_far_sum, "x", swap)
    down_new = adam(adam_down_body, x_at, weights, states, 1, (down_own, down_other), down_shape)
    up_new = adam(adam_up_body, x_at, weights, states, 0, (up_sum, up_other), up_shape)
    return (
        token_grad,
        up_new[0][None],
        down_new[0][None],
        up_new[1][None],
        up_new[2][None],
        down_new[1][None],
        down_new[2][None],
    )


def solution(mesh):
    fine = Mesh(
        mesh.devices.reshape(mesh.devices.shape[0], NX, NY, NC), ("expert", "x", "y", "core")
    )
    every = ("expert", "x", "y", "core")
    dp = ("x", "y", "core")
    state = P("expert", dp, None)
    return jax.shard_map(
        step,
        mesh=fine,
        in_specs=(P(every, None), P(every, None), P(every, None), P(every), P(), P())
        + (state,) * 6,
        out_specs=(P(every, None),) + (state,) * 6,
        check_vma=False,
    )
```

```python
import jax
import jax.numpy as jnp
from jax import lax
from jax.experimental import pallas as pl
from jax.experimental.pallas import tpu as pltpu
from jax.sharding import Mesh
from jax.sharding import PartitionSpec as P


beta_one = 0.9
beta_two = 0.95
bias_one = 1.0 - 0.9**10
bias_two = 1.0 - 0.95**10
rate_value = 0.01
decay_value = 0.1
eps_value = 1e-08

F32 = jnp.float32
BF = jnp.bfloat16
NX, NY, NC = 2, 4, 2
LANE = 128


def row_order():
    return [x * NY * NC + y * NC + c for c in range(NC) for y in range(NY) for x in range(NX)]


def inverse(order):
    back = [0] * len(order)
    for p, r in enumerate(order):
        back[r] = p
    return back


def lanes_taken(value, order):
    width = value.shape[1] // len(order)
    return jnp.concatenate([value[:, r * width : (r + 1) * width] for r in order], axis=1)


def pack_weights_body(up_ref, down_ref, out_ref):
    for g in range(out_ref.shape[0]):
        out_ref[g, 0] = up_ref[:, g * LANE : (g + 1) * LANE].astype(BF)
        out_ref[g, 1] = to_tiles(down_ref[g * 8 : (g + 1) * 8]).astype(BF)


def pack_weights(up, down, groups):
    return pl.pallas_call(
        pack_weights_body,
        out_shape=jax.ShapeDtypeStruct((groups, 2, up.shape[0], LANE), BF),
        name="pack_weights",
    )(up, down)


def unpack_body(in_ref, up_ref, down_ref):
    groups = in_ref.shape[0] // NX
    rows, tall = up_ref.shape[0] // NX, down_ref.shape[0] // NX
    for x in range(NX):
        shares = [in_ref[g * NX + x].astype(F32) for g in range(groups)]
        up = jnp.concatenate([share[0] for share in shares], axis=1)
        up_ref[x * rows : (x + 1) * rows] = lanes_taken(up, row_order()).astype(BF)
        down = jnp.concatenate([from_tiles(share[1]) for share in shares], axis=0)
        down_ref[x * tall : (x + 1) * tall] = down.astype(BF)


def unpack_weights(shares, up_shape, down_shape):
    return pl.pallas_call(
        unpack_body,
        out_shape=(
            jax.ShapeDtypeStruct((NX * up_shape[0], up_shape[1]), BF),
            jax.ShapeDtypeStruct((NX * down_shape[0], down_shape[1]), BF),
        ),
        name="unpack_weights",
    )(shares)


def slot_of_block(ids_ref, own_ref, b):
    mine = ids_ref[b, 0]
    place = jnp.int32(0)
    for e in range(b):
        place = place + (ids_ref[e, 0] == mine).astype(jnp.int32)
    return own_ref[mine] * 2 + place


def dispatch_body(ids_ref, count_ref, own_ref, tok_ref, cot_ref, sx_ref, sdy_ref):
    blocks, rows, _ = tok_ref.shape
    sx_ref[...] = jnp.zeros(sx_ref.shape, BF)
    sdy_ref[...] = jnp.zeros(sdy_ref.shape, BF)
    at = lax.broadcasted_iota(jnp.int32, (rows, 1), 0)
    for b in range(blocks):
        slot = slot_of_block(ids_ref, own_ref, b)
        alive = at < count_ref[b]
        x = jnp.where(alive, tok_ref[b].astype(F32), 0.0)
        dy = jnp.where(alive, cot_ref[b].astype(F32), 0.0)
        sx_ref[slot] = lanes_taken(x, row_order()).astype(BF)
        sdy_ref[slot] = dy.astype(BF)


def smem():
    return pl.BlockSpec(memory_space=pltpu.SMEM)


def vmem():
    return pl.BlockSpec(memory_space=pltpu.VMEM)


def dispatch(ids, count, owner, tokens, cotangent):
    blocks, rows, width = tokens.shape
    out = jax.ShapeDtypeStruct((2 * blocks, rows, width), BF)
    return pl.pallas_call(
        dispatch_body,
        in_specs=[smem(), smem(), smem(), vmem(), vmem()],
        out_shape=(out, out),
        name="dispatch",
    )(ids, count, owner, tokens, cotangent)


def combine_body(ids_ref, own_ref, ret_ref, out_ref):
    for b in range(out_ref.shape[0]):
        slot = slot_of_block(ids_ref, own_ref, b)
        out_ref[b] = lanes_taken(ret_ref[slot].astype(F32), inverse(row_order())).astype(BF)


def combine(ids, owner, returned):
    slots, rows, width = returned.shape
    return pl.pallas_call(
        combine_body,
        in_specs=[smem(), smem(), vmem()],
        out_shape=jax.ShapeDtypeStruct((slots // 2, rows, width), BF),
        name="combine",
    )(ids, owner, returned)


def to_tiles(rows8):
    n = rows8.shape[1] // LANE
    return jnp.concatenate([rows8[:, i * LANE : (i + 1) * LANE] for i in range(n)], axis=0)


def from_tiles(tiles):
    n = tiles.shape[0] // 8
    return jnp.concatenate([tiles[i * 8 : (i + 1) * 8] for i in range(n)], axis=1)


def pack_body(a_ref, b_ref, c_ref, d_ref, out_ref):
    for g in range(out_ref.shape[0]):
        for i, ref in enumerate((a_ref, b_ref)):
            out_ref[g, i] = ref[:, g * LANE : (g + 1) * LANE].astype(BF)
        for i, ref in enumerate((c_ref, d_ref)):
            out_ref[g, 2 + i] = to_tiles(ref[g * 8 : (g + 1) * 8]).astype(BF)


def pack_states(ups, downs, groups):
    rows, cols = ups[0].shape
    return pl.pallas_call(
        pack_body,
        out_shape=jax.ShapeDtypeStruct((groups, 4, rows, cols // groups), BF),
        name="pack_states",
    )(*ups, *downs)


def order_body(old_ref, new_ref, in_ref, out_ref):
    copies = out_ref.shape[0] // in_ref.shape[0]
    for k in range(in_ref.shape[0]):
        for i in range(copies):
            out_ref[new_ref[k] * copies + i] = in_ref[old_ref[k]]


def order_states(old, new, shares, copies):
    shape = (shares.shape[0] * copies,) + shares.shape[1:]
    return pl.pallas_call(
        order_body, in_specs=[smem(), smem(), vmem()], out_shape=jax.ShapeDtypeStruct(shape, BF)
    )(old, new, shares)


def weight_grad_body(half_ref, a_ref, ao_ref, b_ref, bo_ref, out_ref):
    dims = (((0,), (0,)), ((), ()))
    total = lax.dot_general(a_ref[...], b_ref[...], dims, preferred_element_type=F32)
    total += lax.dot_general(ao_ref[...], bo_ref[...], dims, preferred_element_type=F32)
    out_ref[...] = total.astype(BF)


def weight_grad(place, a, a_other, b, b_other, step):
    rows, width = a.shape
    cols = b.shape[1]
    steps = width // 2 // step
    left = pl.BlockSpec(
        (rows, step), lambda i, at: (0, at[0] * steps + lax.rem(at[1] + i, steps))
    )
    right = pl.BlockSpec((rows, cols), lambda i, at: (0, 0))
    return pl.pallas_call(
        weight_grad_body,
        grid_spec=pltpu.PrefetchScalarGridSpec(
            num_scalar_prefetch=1,
            grid=(steps,),
            in_specs=[left, left, right, right],
            out_specs=pl.BlockSpec((step, cols), lambda i, at: (i, 0)),
        ),
        out_shape=jax.ShapeDtypeStruct((width // 2, cols), BF),
    )(place, a, a_other, b, b_other)


def flip_body(core_ref, own_ref, other_ref, out_ref):
    rows = own_ref.shape[0]
    out_ref[:, 0:rows] = own_ref[...].astype(F32).T.astype(BF)
    out_ref[:, rows : 2 * rows] = other_ref[...].astype(F32).T.astype(BF)


def flip(place, own, other, step=256):
    rows, width = own.shape
    steps = width // 2 // step
    part = pl.BlockSpec((rows, step), lambda i, at: (0, at[0] * steps + i))
    return pl.pallas_call(
        flip_body,
        grid_spec=pltpu.PrefetchScalarGridSpec(
            num_scalar_prefetch=1,
            grid=(steps,),
            in_specs=[part, part],
            out_specs=pl.BlockSpec((step, 2 * rows), lambda i, at: (i, 0)),
        ),
        out_shape=jax.ShapeDtypeStruct((width // 2, 2 * rows), BF),
        name="flip",
    )(place, own, other)


def up_grad_body(xt_ref, own_ref, other_ref, out_ref):
    rows = own_ref.shape[0]
    total = jnp.dot(xt_ref[:, 0:rows], own_ref[...], preferred_element_type=F32)
    total += jnp.dot(xt_ref[:, rows : 2 * rows], other_ref[...], preferred_element_type=F32)
    out_ref[...] = total.astype(BF)


def up_grad_part(flipped, own, other, steps=4):
    width, deep = flipped.shape
    rows, cols = own.shape
    right = pl.BlockSpec((rows, cols), lambda i: (0, 0))
    return pl.pallas_call(
        up_grad_body,
        grid=(steps,),
        in_specs=[pl.BlockSpec((width // steps, deep), lambda i: (i, 0)), right, right],
        out_specs=pl.BlockSpec((width // steps, cols), lambda i: (i, 0)),
        out_shape=jax.ShapeDtypeStruct((width, cols), BF),
        name="up_part",
    )(flipped, own, other)


def back_body(at_ref, dy_ref, slopes_ref, *refs):
    pieces, out_ref = refs[:-1], refs[-1]
    dims = (((1,), (1,)), ((), ()))
    per_core = len(pieces) // NC
    dy = dy_ref[...]
    for k in range(NC):
        own, above, low, high, below = (p[...] for p in pieces[k * per_core : (k + 1) * per_core])
        core = at_ref[0] if k == 0 else 1 - at_ref[0]
        for first, group in ((0, [own, above]), (2, [low, high, below])):
            both = lax.dot_general(
                dy, jnp.concatenate(group, axis=0), dims, preferred_element_type=F32
            )
            for i in range(2):
                tile = core * NY + lax.rem(at_ref[1] + first + i, NY)
                lanes = pl.ds(pl.multiple_of(tile * LANE, LANE), LANE)
                value = both[:, i * LANE : (i + 1) * LANE] * slopes_ref[:, lanes]
                out_ref[:, lanes] = value.astype(BF)


def back_grad(place, dy, slopes, pieces):
    return pl.pallas_call(
        back_body,
        in_specs=[smem(), vmem(), vmem()] + [vmem()] * len(pieces),
        out_shape=jax.ShapeDtypeStruct(slopes.shape, BF),
        name="back",
    )(place, dy, slopes, *pieces)


def relay_body(part_ref, below_ref, above_ref, up_ref, down_ref):
    tall = below_ref.shape[0]
    wide = 2 * tall
    mine = part_ref[wide : 2 * wide].astype(F32)
    up_ref[0:tall] = (mine[0:tall] + below_ref[...].astype(F32)).astype(BF)
    up_ref[tall:wide] = part_ref[wide + tall : 2 * wide]
    mine = part_ref[3 * wide + tall : 4 * wide].astype(F32)
    down_ref[0:tall] = part_ref[3 * wide : 3 * wide + tall]
    down_ref[tall:wide] = (mine + above_ref[...].astype(F32)).astype(BF)


def relay(part, below, above):
    tall, cols = below.shape
    out = jax.ShapeDtypeStruct((2 * tall, cols), BF)
    return pl.pallas_call(relay_body, out_shape=(out, out), name="relay")(part, below, above)


def finish_body(x_ref, part_ref, below_ref, above_ref, own_ref, send_ref):
    tall = own_ref.shape[0]
    total = part_ref[...].astype(F32) + below_ref[...].astype(F32) + above_ref[...].astype(F32)
    low, high = total[0:tall], total[tall : 2 * tall]
    first = x_ref[0] == 0
    own_ref[...] = jnp.where(first, low, high)
    send_ref[...] = jnp.where(first, high, low).astype(BF)


def finish(x_at, part, below, above):
    wide, cols = below.shape
    whole = pl.BlockSpec((wide, cols), lambda i: (0, 0))
    half_spec = pl.BlockSpec((wide // 2, cols), lambda i: (0, 0))
    return pl.pallas_call(
        finish_body,
        grid=(1,),
        in_specs=[smem(), whole, whole, whole],
        out_specs=(half_spec, half_spec),
        out_shape=(
            jax.ShapeDtypeStruct((wide // 2, cols), F32),
            jax.ShapeDtypeStruct((wide // 2, cols), BF),
        ),
        name="finish",
    )(x_at, part, below, above)


def adam_update(weight, moment, second, gradient):
    moment_new = beta_one * moment + (1.0 - beta_one) * gradient
    second_new = beta_two * second + (1.0 - beta_two) * gradient * gradient
    update = moment_new / bias_one / (jnp.sqrt(second_new / bias_two) + eps_value)
    return (weight - rate_value * (update + decay_value * weight), moment_new, second_new)


def adam_up_body(x_ref, weight_ref, state_ref, grad_ref, other_ref, *outs):
    rows = other_ref.shape[0]
    own = grad_ref[pl.ds(pl.multiple_of(x_ref[0] * rows, 16), rows)]
    both = own.astype(F32) + other_ref[...].astype(F32)
    grad = lanes_taken(both, inverse(row_order()))
    for g in range(state_ref.shape[0]):
        lanes = slice(g * LANE, (g + 1) * LANE)
        m, v = (state_ref[g, i].astype(F32) for i in range(2))
        w = weight_ref[g * NX + x_ref[0], 0].astype(F32)
        for ref, value in zip(outs, adam_update(w, m, v, grad[:, lanes])):
            ref[:, lanes] = value


def adam_down_body(x_ref, weight_ref, state_ref, grad_ref, other_ref, *outs):
    for g in range(state_ref.shape[0]):
        rows = slice(g * 8, (g + 1) * 8)
        m, v = (from_tiles(state_ref[g, i].astype(F32)) for i in range(2))
        w = from_tiles(weight_ref[g * NX + x_ref[0], 0].astype(F32))
        grad = grad_ref[rows] + other_ref[rows].astype(F32)
        for ref, value in zip(outs, adam_update(w, m, v, grad)):
            ref[rows] = value


def adam(body, x_at, weights, states, which, grads, shape):
    groups, _, rows, wide = states.shape
    full = pl.BlockSpec(shape, lambda i: (0, 0))
    return pl.pallas_call(
        body,
        grid=(1,),
        in_specs=[
            smem(),
            pl.BlockSpec((weights.shape[0], 1, rows, wide), lambda i: (0, which, 0, 0)),
            pl.BlockSpec((groups, 2, rows, wide), lambda i: (0, which, 0, 0)),
        ]
        + [pl.BlockSpec(g.shape, lambda i: (0, 0)) for g in grads],
        out_specs=[full] * 3,
        out_shape=[jax.ShapeDtypeStruct(shape, F32)] * 3,
    )(x_at, weights, states, *grads)


def silu_parts(pre_act):
    sigma = jax.nn.sigmoid(pre_act)
    return (pre_act * sigma, sigma * (1.0 + pre_act * (1.0 - sigma)))


def exchange(array, axis):
    return lax.all_to_all(array, axis, split_axis=0, concat_axis=0, tiled=True)


def from_partner(array):
    return lax.ppermute(array, "core", [(0, 1), (1, 0)])


def step(
    tokens,
    cotangent,
    block_expert,
    block_count,
    old_owner,
    new_owner,
    up_weight,
    down_weight,
    up_first,
    up_second,
    down_first,
    down_second,
):
    groups = lax.axis_size("expert")
    tok_rows, features = tokens.shape
    blocks = block_count.shape[0]
    rows = tok_rows // blocks
    core_at = lax.axis_index("core").astype(jnp.int32)
    y_at = lax.axis_index("y").astype(jnp.int32)
    x_at = lax.axis_index("x").astype(jnp.int32).reshape(1)
    down_place = jnp.stack([core_at, y_at])
    up_shape, down_shape = up_weight.shape[1:], down_weight.shape[1:]

    packed = pack_weights(up_weight[0], down_weight[0], groups)
    spread = exchange(packed, "expert")
    ordered = order_states(old_owner, new_owner, spread, NX)
    weights = exchange(ordered, ("expert", "x"))
    up_pair, down_pair = unpack_weights(weights, up_shape, down_shape)
    up_mat = lax.all_gather(up_pair, ("core", "y"), axis=0, tiled=True)
    rising = [(i, (i + 1) % NY) for i in range(NY)]
    falling = [(i, (i - 1) % NY) for i in range(NY)]
    tall = down_shape[0]
    w_below = lax.ppermute(down_pair, "y", rising)
    w_above = lax.ppermute(down_pair, "y", falling)
    w_low = lax.ppermute(w_below[:tall], "y", rising)
    w_high = lax.ppermute(w_above[tall:], "y", falling)
    pieces = (down_pair, w_above, w_low, w_high, w_below)
    pieces += tuple(from_partner(piece) for piece in pieces)

    send_x, send_dy = dispatch(
        block_expert,
        block_count,
        new_owner,
        tokens.reshape(blocks, rows, features),
        cotangent.reshape(blocks, rows, features),
    )
    send_x, _ = lax.optimization_barrier((send_x, down_pair))
    inputs = exchange(send_x, "expert")
    send_dy, inputs = lax.optimization_barrier((send_dy, inputs))
    inputs = inputs.reshape(-1, features)
    upstream = exchange(send_dy, "expert").reshape(-1, features)
    inputs_other, upstream_other = from_partner(inputs), from_partner(upstream)

    flipped = flip(down_place, inputs, inputs_other)

    packed = pack_states(
        (up_first[0], up_second[0]), (down_first[0], down_second[0]), groups
    )
    packed, upstream, flipped = lax.optimization_barrier((packed, upstream, flipped))
    shares = exchange(packed, "expert")

    pre_act = jnp.dot(inputs, up_mat, preferred_element_type=F32)
    active, slopes = silu_parts(pre_act)
    hidden = active.astype(BF)
    hidden_other = from_partner(hidden)
    down_part = weight_grad(down_place, hidden, hidden_other, upstream, upstream_other, 128)
    below = lax.ppermute(down_part[4 * tall : 5 * tall], "y", rising)
    above = lax.ppermute(down_part[5 * tall : 6 * tall], "y", falling)
    slopes, _ = lax.optimization_barrier((slopes, down_part))
    pre_grad = back_grad(down_place, upstream, slopes, pieces)
    pre_grad_other = from_partner(pre_grad)
    up_part = up_grad_part(flipped, pre_grad, pre_grad_other)
    up_sum = lax.psum_scatter(up_part, "y", scatter_dimension=0, tiled=True)
    ordered = order_states(old_owner, new_owner, shares, 1)
    ordered, up_part, pre_grad, down_part = lax.optimization_barrier(
        (ordered, up_part, pre_grad, down_part)
    )
    states = exchange(ordered, "expert")
    going_up, going_down = relay(down_part, below, above)
    below = lax.ppermute(going_up, "y", rising)
    above = lax.ppermute(going_down, "y", falling)
    input_grad = lax.dot_general(
        pre_grad, up_mat, (((1,), (1,)), ((), ())), preferred_element_type=F32
    ).astype(BF)
    input_grad, states = lax.optimization_barrier((input_grad, states))
    returned = exchange(input_grad.reshape(-1, rows, features), "expert")
    token_grad = combine(block_expert, new_owner, returned).reshape(tok_rows, features)

    swap = [(0, 1), (1, 0)]
    down_own, down_send = finish(x_at, down_part, below, above)
    down_other = lax.ppermute(down_send, "x", swap)
    up_send = lax.dynamic_slice_in_dim(up_sum, (1 - x_at[0]) * up_shape[0], up_shape[0])
    up_other = lax.ppermute(up_send, "x", swap)
    down_new = adam(adam_down_body, x_at, weights, states, 1, (down_own, down_other), down_shape)
    up_new = adam(adam_up_body, x_at, weights, states, 0, (up_sum, up_other), up_shape)
    return (
        token_grad,
        up_new[0][None],
        down_new[0][None],
        up_new[1][None],
        up_new[2][None],
        down_new[1][None],
        down_new[2][None],
    )


def solution(mesh):
    fine = Mesh(
        mesh.devices.reshape(mesh.devices.shape[0], NX, NY, NC), ("expert", "x", "y", "core")
    )
    every = ("expert", "x", "y", "core")
    dp = ("x", "y", "core")
    state = P("expert", dp, None)
    return jax.shard_map(
        step,
        mesh=fine,
        in_specs=(P(every, None), P(every, None), P(every, None), P(every), P(), P())
        + (state,) * 6,
        out_specs=(P(every, None),) + (state,) * 6,
        check_vma=False,
    )
```

```python
import jax
import jax.numpy as jnp
from jax import lax
from jax.experimental import pallas as pl
from jax.experimental.pallas import tpu as pltpu
from jax.sharding import Mesh
from jax.sharding import PartitionSpec as P


beta_one = 0.9
beta_two = 0.95
bias_one = 1.0 - 0.9**10
bias_two = 1.0 - 0.95**10
rate_value = 0.01
decay_value = 0.1
eps_value = 1e-08

F32 = jnp.float32
BF = jnp.bfloat16
NX, NY, NC = 2, 4, 2
LANE = 128


def row_order():
    return [x * NY * NC + y * NC + c for c in range(NC) for y in range(NY) for x in range(NX)]


def inverse(order):
    back = [0] * len(order)
    for p, r in enumerate(order):
        back[r] = p
    return back


def lanes_taken(value, order):
    width = value.shape[1] // len(order)
    return jnp.concatenate([value[:, r * width : (r + 1) * width] for r in order], axis=1)


def pack_weights_body(up_ref, down_ref, out_ref):
    for g in range(out_ref.shape[0]):
        out_ref[g, 0] = up_ref[:, g * LANE : (g + 1) * LANE].astype(BF)
        out_ref[g, 1] = to_tiles(down_ref[g * 8 : (g + 1) * 8]).astype(BF)


def pack_weights(up, down, groups):
    return pl.pallas_call(
        pack_weights_body,
        out_shape=jax.ShapeDtypeStruct((groups, 2, up.shape[0], LANE), BF),
        name="pack_weights",
    )(up, down)


def unpack_body(in_ref, up_ref, down_ref):
    groups = in_ref.shape[0] // NX
    rows, tall = up_ref.shape[0] // NX, down_ref.shape[0] // NX
    for x in range(NX):
        shares = [in_ref[g * NX + x].astype(F32) for g in range(groups)]
        up = jnp.concatenate([share[0] for share in shares], axis=1)
        up_ref[x * rows : (x + 1) * rows] = lanes_taken(up, row_order()).astype(BF)
        down = jnp.concatenate([from_tiles(share[1]) for share in shares], axis=0)
        down_ref[x * tall : (x + 1) * tall] = down.astype(BF)


def unpack_weights(shares, up_shape, down_shape):
    return pl.pallas_call(
        unpack_body,
        out_shape=(
            jax.ShapeDtypeStruct((NX * up_shape[0], up_shape[1]), BF),
            jax.ShapeDtypeStruct((NX * down_shape[0], down_shape[1]), BF),
        ),
        name="unpack_weights",
    )(shares)


def slot_of_block(ids_ref, own_ref, b):
    mine = ids_ref[b, 0]
    place = jnp.int32(0)
    for e in range(b):
        place = place + (ids_ref[e, 0] == mine).astype(jnp.int32)
    return own_ref[mine] * 2 + place


def dispatch_body(ids_ref, count_ref, own_ref, tok_ref, cot_ref, sx_ref, sdy_ref):
    blocks, rows, _ = tok_ref.shape
    sx_ref[...] = jnp.zeros(sx_ref.shape, BF)
    sdy_ref[...] = jnp.zeros(sdy_ref.shape, BF)
    at = lax.broadcasted_iota(jnp.int32, (rows, 1), 0)
    for b in range(blocks):
        slot = slot_of_block(ids_ref, own_ref, b)
        alive = at < count_ref[b]
        x = jnp.where(alive, tok_ref[b].astype(F32), 0.0)
        dy = jnp.where(alive, cot_ref[b].astype(F32), 0.0)
        sx_ref[slot] = lanes_taken(x, row_order()).astype(BF)
        sdy_ref[slot] = dy.astype(BF)


def smem():
    return pl.BlockSpec(memory_space=pltpu.SMEM)


def vmem():
    return pl.BlockSpec(memory_space=pltpu.VMEM)


def dispatch(ids, count, owner, tokens, cotangent):
    blocks, rows, width = tokens.shape
    out = jax.ShapeDtypeStruct((2 * blocks, rows, width), BF)
    return pl.pallas_call(
        dispatch_body,
        in_specs=[smem(), smem(), smem(), vmem(), vmem()],
        out_shape=(out, out),
        name="dispatch",
    )(ids, count, owner, tokens, cotangent)


def combine_body(ids_ref, own_ref, ret_ref, out_ref):
    for b in range(out_ref.shape[0]):
        slot = slot_of_block(ids_ref, own_ref, b)
        out_ref[b] = lanes_taken(ret_ref[slot].astype(F32), inverse(row_order())).astype(BF)


def combine(ids, owner, returned):
    slots, rows, width = returned.shape
    return pl.pallas_call(
        combine_body,
        in_specs=[smem(), smem(), vmem()],
        out_shape=jax.ShapeDtypeStruct((slots // 2, rows, width), BF),
        name="combine",
    )(ids, owner, returned)


def to_tiles(rows8):
    n = rows8.shape[1] // LANE
    return jnp.concatenate([rows8[:, i * LANE : (i + 1) * LANE] for i in range(n)], axis=0)


def from_tiles(tiles):
    n = tiles.shape[0] // 8
    return jnp.concatenate([tiles[i * 8 : (i + 1) * 8] for i in range(n)], axis=1)


def pack_body(a_ref, b_ref, c_ref, d_ref, out_ref):
    for g in range(out_ref.shape[0]):
        for i, ref in enumerate((a_ref, b_ref)):
            out_ref[g, i] = ref[:, g * LANE : (g + 1) * LANE].astype(BF)
        for i, ref in enumerate((c_ref, d_ref)):
            out_ref[g, 2 + i] = to_tiles(ref[g * 8 : (g + 1) * 8]).astype(BF)


def pack_states(ups, downs, groups):
    rows, cols = ups[0].shape
    return pl.pallas_call(
        pack_body,
        out_shape=jax.ShapeDtypeStruct((groups, 4, rows, cols // groups), BF),
        name="pack_states",
    )(*ups, *downs)


def order_body(old_ref, new_ref, in_ref, out_ref):
    copies = out_ref.shape[0] // in_ref.shape[0]
    for k in range(in_ref.shape[0]):
        for i in range(copies):
            out_ref[new_ref[k] * copies + i] = in_ref[old_ref[k]]


def order_states(old, new, shares, copies):
    shape = (shares.shape[0] * copies,) + shares.shape[1:]
    return pl.pallas_call(
        order_body, in_specs=[smem(), smem(), vmem()], out_shape=jax.ShapeDtypeStruct(shape, BF)
    )(old, new, shares)


def weight_grad_body(half_ref, a_ref, ao_ref, b_ref, bo_ref, out_ref):
    dims = (((0,), (0,)), ((), ()))
    total = lax.dot_general(a_ref[...], b_ref[...], dims, preferred_element_type=F32)
    total += lax.dot_general(ao_ref[...], bo_ref[...], dims, preferred_element_type=F32)
    out_ref[...] = total.astype(BF)


def weight_grad(place, a, a_other, b, b_other, step):
    rows, width = a.shape
    cols = b.shape[1]
    steps = width // 2 // step
    left = pl.BlockSpec(
        (rows, step), lambda i, at: (0, at[0] * steps + lax.rem(at[1] + i, steps))
    )
    right = pl.BlockSpec((rows, cols), lambda i, at: (0, 0))
    return pl.pallas_call(
        weight_grad_body,
        grid_spec=pltpu.PrefetchScalarGridSpec(
            num_scalar_prefetch=1,
            grid=(steps,),
            in_specs=[left, left, right, right],
            out_specs=pl.BlockSpec((step, cols), lambda i, at: (i, 0)),
        ),
        out_shape=jax.ShapeDtypeStruct((width // 2, cols), BF),
    )(place, a, a_other, b, b_other)


def flip_body(core_ref, own_ref, other_ref, out_ref):
    rows = own_ref.shape[0]
    out_ref[:, 0:rows] = own_ref[...].astype(F32).T.astype(BF)
    out_ref[:, rows : 2 * rows] = other_ref[...].astype(F32).T.astype(BF)


def flip(place, own, other, step=256):
    rows, width = own.shape
    steps = width // 2 // step
    part = pl.BlockSpec((rows, step), lambda i, at: (0, at[0] * steps + i))
    return pl.pallas_call(
        flip_body,
        grid_spec=pltpu.PrefetchScalarGridSpec(
            num_scalar_prefetch=1,
            grid=(steps,),
            in_specs=[part, part],
            out_specs=pl.BlockSpec((step, 2 * rows), lambda i, at: (i, 0)),
        ),
        out_shape=jax.ShapeDtypeStruct((width // 2, 2 * rows), BF),
        name="flip",
    )(place, own, other)


def up_grad_body(xt_ref, own_ref, other_ref, out_ref):
    rows = own_ref.shape[0]
    total = jnp.dot(xt_ref[:, 0:rows], own_ref[...], preferred_element_type=F32)
    total += jnp.dot(xt_ref[:, rows : 2 * rows], other_ref[...], preferred_element_type=F32)
    out_ref[...] = total.astype(BF)


def up_grad_part(flipped, own, other, steps=4):
    width, deep = flipped.shape
    rows, cols = own.shape
    right = pl.BlockSpec((rows, cols), lambda i: (0, 0))
    return pl.pallas_call(
        up_grad_body,
        grid=(steps,),
        in_specs=[pl.BlockSpec((width // steps, deep), lambda i: (i, 0)), right, right],
        out_specs=pl.BlockSpec((width // steps, cols), lambda i: (i, 0)),
        out_shape=jax.ShapeDtypeStruct((width, cols), BF),
        name="up_part",
    )(flipped, own, other)


def relay_body(part_ref, below_ref, above_ref, up_ref, down_ref):
    tall = below_ref.shape[0]
    wide = 2 * tall
    mine = part_ref[wide : 2 * wide].astype(F32)
    up_ref[0:tall] = (mine[0:tall] + below_ref[...].astype(F32)).astype(BF)
    up_ref[tall:wide] = part_ref[wide + tall : 2 * wide]
    mine = part_ref[3 * wide + tall : 4 * wide].astype(F32)
    down_ref[0:tall] = part_ref[3 * wide : 3 * wide + tall]
    down_ref[tall:wide] = (mine + above_ref[...].astype(F32)).astype(BF)


def relay(part, below, above):
    tall, cols = below.shape
    out = jax.ShapeDtypeStruct((2 * tall, cols), BF)
    return pl.pallas_call(relay_body, out_shape=(out, out), name="relay")(part, below, above)


def finish_body(x_ref, part_ref, below_ref, above_ref, own_ref, send_ref):
    tall = own_ref.shape[0]
    total = part_ref[...].astype(F32) + below_ref[...].astype(F32) + above_ref[...].astype(F32)
    low, high = total[0:tall], total[tall : 2 * tall]
    first = x_ref[0] == 0
    own_ref[...] = jnp.where(first, low, high)
    send_ref[...] = jnp.where(first, high, low).astype(BF)


def finish(x_at, part, below, above):
    wide, cols = below.shape
    whole = pl.BlockSpec((wide, cols), lambda i: (0, 0))
    half_spec = pl.BlockSpec((wide // 2, cols), lambda i: (0, 0))
    return pl.pallas_call(
        finish_body,
        grid=(1,),
        in_specs=[smem(), whole, whole, whole],
        out_specs=(half_spec, half_spec),
        out_shape=(
            jax.ShapeDtypeStruct((wide // 2, cols), F32),
            jax.ShapeDtypeStruct((wide // 2, cols), BF),
        ),
        name="finish",
    )(x_at, part, below, above)


def adam_update(weight, moment, second, gradient):
    moment_new = beta_one * moment + (1.0 - beta_one) * gradient
    second_new = beta_two * second + (1.0 - beta_two) * gradient * gradient
    update = moment_new / bias_one / (jnp.sqrt(second_new / bias_two) + eps_value)
    return (weight - rate_value * (update + decay_value * weight), moment_new, second_new)


def adam_up_body(x_ref, weight_ref, state_ref, grad_ref, other_ref, *outs):
    rows = other_ref.shape[0]
    own = grad_ref[pl.ds(pl.multiple_of(x_ref[0] * rows, 16), rows)]
    both = own.astype(F32) + other_ref[...].astype(F32)
    grad = lanes_taken(both, inverse(row_order()))
    for g in range(state_ref.shape[0]):
        lanes = slice(g * LANE, (g + 1) * LANE)
        m, v = (state_ref[g, i].astype(F32) for i in range(2))
        w = weight_ref[g * NX + x_ref[0], 0].astype(F32)
        for ref, value in zip(outs, adam_update(w, m, v, grad[:, lanes])):
            ref[:, lanes] = value


def adam_down_body(x_ref, weight_ref, state_ref, grad_ref, other_ref, *outs):
    for g in range(state_ref.shape[0]):
        rows = slice(g * 8, (g + 1) * 8)
        m, v = (from_tiles(state_ref[g, i].astype(F32)) for i in range(2))
        w = from_tiles(weight_ref[g * NX + x_ref[0], 0].astype(F32))
        grad = grad_ref[rows] + other_ref[rows].astype(F32)
        for ref, value in zip(outs, adam_update(w, m, v, grad)):
            ref[rows] = value


def adam(body, x_at, weights, states, which, grads, shape):
    groups, _, rows, wide = states.shape
    full = pl.BlockSpec(shape, lambda i: (0, 0))
    return pl.pallas_call(
        body,
        grid=(1,),
        in_specs=[
            smem(),
            pl.BlockSpec((weights.shape[0], 1, rows, wide), lambda i: (0, which, 0, 0)),
            pl.BlockSpec((groups, 2, rows, wide), lambda i: (0, which, 0, 0)),
        ]
        + [pl.BlockSpec(g.shape, lambda i: (0, 0)) for g in grads],
        out_specs=[full] * 3,
        out_shape=[jax.ShapeDtypeStruct(shape, F32)] * 3,
    )(x_at, weights, states, *grads)


def silu_parts(pre_act):
    sigma = jax.nn.sigmoid(pre_act)
    return (pre_act * sigma, sigma * (1.0 + pre_act * (1.0 - sigma)))


def exchange(array, axis):
    return lax.all_to_all(array, axis, split_axis=0, concat_axis=0, tiled=True)


def from_partner(array):
    return lax.ppermute(array, "core", [(0, 1), (1, 0)])


def step(
    tokens,
    cotangent,
    block_expert,
    block_count,
    old_owner,
    new_owner,
    up_weight,
    down_weight,
    up_first,
    up_second,
    down_first,
    down_second,
):
    groups = lax.axis_size("expert")
    tok_rows, features = tokens.shape
    blocks = block_count.shape[0]
    rows = tok_rows // blocks
    core_at = lax.axis_index("core").astype(jnp.int32)
    y_at = lax.axis_index("y").astype(jnp.int32)
    x_at = lax.axis_index("x").astype(jnp.int32).reshape(1)
    down_place = jnp.stack([core_at, y_at])
    up_shape, down_shape = up_weight.shape[1:], down_weight.shape[1:]

    packed = pack_weights(up_weight[0], down_weight[0], groups)
    spread = exchange(packed, "expert")
    ordered = order_states(old_owner, new_owner, spread, NX)
    weights = exchange(ordered, ("expert", "x"))
    up_pair, down_pair = unpack_weights(weights, up_shape, down_shape)
    up_mat = lax.all_gather(up_pair, ("core", "y"), axis=0, tiled=True)
    down_mat = lax.all_gather(down_pair, ("core", "y"), axis=0, tiled=True)

    send_x, send_dy = dispatch(
        block_expert,
        block_count,
        new_owner,
        tokens.reshape(blocks, rows, features),
        cotangent.reshape(blocks, rows, features),
    )
    send_x, _ = lax.optimization_barrier((send_x, down_pair))
    inputs = exchange(send_x, "expert")
    send_dy, inputs = lax.optimization_barrier((send_dy, inputs))
    inputs = inputs.reshape(-1, features)
    upstream = exchange(send_dy, "expert").reshape(-1, features)
    inputs_other, upstream_other = from_partner(inputs), from_partner(upstream)

    flipped = flip(down_place, inputs, inputs_other)

    packed = pack_states(
        (up_first[0], up_second[0]), (down_first[0], down_second[0]), groups
    )
    packed, upstream, flipped = lax.optimization_barrier((packed, upstream, flipped))
    shares = exchange(packed, "expert")

    pre_act = jnp.dot(inputs, up_mat, preferred_element_type=F32)
    active, slopes = silu_parts(pre_act)
    hidden = active.astype(BF)
    hidden_other = from_partner(hidden)
    down_part = weight_grad(down_place, hidden, hidden_other, upstream, upstream_other, 128)
    tall = down_shape[0]
    rising = [(i, (i + 1) % NY) for i in range(NY)]
    falling = [(i, (i - 1) % NY) for i in range(NY)]
    below = lax.ppermute(down_part[4 * tall : 5 * tall], "y", rising)
    above = lax.ppermute(down_part[5 * tall : 6 * tall], "y", falling)
    upstream, _ = lax.optimization_barrier((upstream, down_part))
    back = lax.dot_general(upstream, down_mat, (((1,), (1,)), ((), ())), preferred_element_type=F32)
    pre_grad = (back * slopes).astype(BF)
    pre_grad_other = from_partner(pre_grad)
    down_part, pre_grad = lax.optimization_barrier((down_part, pre_grad))
    going_up, going_down = relay(down_part, below, above)
    below = lax.ppermute(going_up, "y", rising)
    above = lax.ppermute(going_down, "y", falling)
    up_part = up_grad_part(flipped, pre_grad, pre_grad_other)
    up_sum = lax.psum_scatter(up_part, "y", scatter_dimension=0, tiled=True)
    ordered = order_states(old_owner, new_owner, shares, 1)
    ordered, up_part, pre_grad = lax.optimization_barrier((ordered, up_part, pre_grad))
    states = exchange(ordered, "expert")
    input_grad = lax.dot_general(
        pre_grad, up_mat, (((1,), (1,)), ((), ())), preferred_element_type=F32
    ).astype(BF)
    input_grad, states = lax.optimization_barrier((input_grad, states))
    returned = exchange(input_grad.reshape(-1, rows, features), "expert")
    token_grad = combine(block_expert, new_owner, returned).reshape(tok_rows, features)

    swap = [(0, 1), (1, 0)]
    down_own, down_send = finish(x_at, down_part, below, above)
    down_other = lax.ppermute(down_send, "x", swap)
    up_send = lax.dynamic_slice_in_dim(up_sum, (1 - x_at[0]) * up_shape[0], up_shape[0])
    up_other = lax.ppermute(up_send, "x", swap)
    down_new = adam(adam_down_body, x_at, weights, states, 1, (down_own, down_other), down_shape)
    up_new = adam(adam_up_body, x_at, weights, states, 0, (up_sum, up_other), up_shape)
    return (
        token_grad,
        up_new[0][None],
        down_new[0][None],
        up_new[1][None],
        up_new[2][None],
        down_new[1][None],
        down_new[2][None],
    )


def solution(mesh):
    fine = Mesh(
        mesh.devices.reshape(mesh.devices.shape[0], NX, NY, NC), ("expert", "x", "y", "core")
    )
    every = ("expert", "x", "y", "core")
    dp = ("x", "y", "core")
    state = P("expert", dp, None)
    return jax.shard_map(
        step,
        mesh=fine,
        in_specs=(P(every, None), P(every, None), P(every, None), P(every), P(), P())
        + (state,) * 6,
        out_specs=(P(every, None),) + (state,) * 6,
        check_vma=False,
    )
```

```python
import jax
import jax.numpy as jnp
from jax import lax
from jax.experimental import pallas as pl
from jax.experimental.pallas import tpu as pltpu
from jax.sharding import Mesh
from jax.sharding import PartitionSpec as P


beta_one = 0.9
beta_two = 0.95
bias_one = 1.0 - 0.9**10
bias_two = 1.0 - 0.95**10
rate_value = 0.01
decay_value = 0.1
eps_value = 1e-08

F32 = jnp.float32
BF = jnp.bfloat16
NX, NY, NC = 2, 4, 2
LANE = 128


def row_order():
    return [x * NY * NC + y * NC + c for c in range(NC) for y in range(NY) for x in range(NX)]


def inverse(order):
    back = [0] * len(order)
    for p, r in enumerate(order):
        back[r] = p
    return back


def lanes_taken(value, order):
    width = value.shape[1] // len(order)
    return jnp.concatenate([value[:, r * width : (r + 1) * width] for r in order], axis=1)


def pack_weights_body(up_ref, down_ref, out_ref):
    for g in range(out_ref.shape[0]):
        out_ref[g, 0] = up_ref[:, g * LANE : (g + 1) * LANE].astype(BF)
        out_ref[g, 1] = to_tiles(down_ref[g * 8 : (g + 1) * 8]).astype(BF)


def pack_weights(up, down, groups):
    return pl.pallas_call(
        pack_weights_body,
        out_shape=jax.ShapeDtypeStruct((groups, 2, up.shape[0], LANE), BF),
        name="pack_weights",
    )(up, down)


def unpack_body(in_ref, up_ref, down_ref):
    groups = in_ref.shape[0] // NX
    rows, tall = up_ref.shape[0] // NX, down_ref.shape[0] // NX
    for x in range(NX):
        shares = [in_ref[g * NX + x].astype(F32) for g in range(groups)]
        up = jnp.concatenate([share[0] for share in shares], axis=1)
        up_ref[x * rows : (x + 1) * rows] = lanes_taken(up, row_order()).astype(BF)
        down = jnp.concatenate([from_tiles(share[1]) for share in shares], axis=0)
        down_ref[x * tall : (x + 1) * tall] = down.astype(BF)


def unpack_weights(shares, up_shape, down_shape):
    return pl.pallas_call(
        unpack_body,
        out_shape=(
            jax.ShapeDtypeStruct((NX * up_shape[0], up_shape[1]), BF),
            jax.ShapeDtypeStruct((NX * down_shape[0], down_shape[1]), BF),
        ),
        name="unpack_weights",
    )(shares)


def slot_of_block(ids_ref, own_ref, b):
    mine = ids_ref[b, 0]
    place = jnp.int32(0)
    for e in range(b):
        place = place + (ids_ref[e, 0] == mine).astype(jnp.int32)
    return own_ref[mine] * 2 + place


def dispatch_body(ids_ref, count_ref, own_ref, tok_ref, cot_ref, sx_ref, sdy_ref):
    blocks, rows, _ = tok_ref.shape
    sx_ref[...] = jnp.zeros(sx_ref.shape, BF)
    sdy_ref[...] = jnp.zeros(sdy_ref.shape, BF)
    at = lax.broadcasted_iota(jnp.int32, (rows, 1), 0)
    for b in range(blocks):
        slot = slot_of_block(ids_ref, own_ref, b)
        alive = at < count_ref[b]
        x = jnp.where(alive, tok_ref[b].astype(F32), 0.0)
        dy = jnp.where(alive, cot_ref[b].astype(F32), 0.0)
        sx_ref[slot] = lanes_taken(x, row_order()).astype(BF)
        sdy_ref[slot] = dy.astype(BF)


def smem():
    return pl.BlockSpec(memory_space=pltpu.SMEM)


def vmem():
    return pl.BlockSpec(memory_space=pltpu.VMEM)


def dispatch(ids, count, owner, tokens, cotangent):
    blocks, rows, width = tokens.shape
    out = jax.ShapeDtypeStruct((2 * blocks, rows, width), BF)
    return pl.pallas_call(
        dispatch_body,
        in_specs=[smem(), smem(), smem(), vmem(), vmem()],
        out_shape=(out, out),
        name="dispatch",
    )(ids, count, owner, tokens, cotangent)


def combine_body(ids_ref, own_ref, ret_ref, out_ref):
    for b in range(out_ref.shape[0]):
        slot = slot_of_block(ids_ref, own_ref, b)
        out_ref[b] = lanes_taken(ret_ref[slot].astype(F32), inverse(row_order())).astype(BF)


def combine(ids, owner, returned):
    slots, rows, width = returned.shape
    return pl.pallas_call(
        combine_body,
        in_specs=[smem(), smem(), vmem()],
        out_shape=jax.ShapeDtypeStruct((slots // 2, rows, width), BF),
        name="combine",
    )(ids, owner, returned)


def to_tiles(rows8):
    n = rows8.shape[1] // LANE
    return jnp.concatenate([rows8[:, i * LANE : (i + 1) * LANE] for i in range(n)], axis=0)


def from_tiles(tiles):
    n = tiles.shape[0] // 8
    return jnp.concatenate([tiles[i * 8 : (i + 1) * 8] for i in range(n)], axis=1)


def pack_body(a_ref, b_ref, c_ref, d_ref, out_ref):
    for g in range(out_ref.shape[0]):
        for i, ref in enumerate((a_ref, b_ref)):
            out_ref[g, i] = ref[:, g * LANE : (g + 1) * LANE].astype(BF)
        for i, ref in enumerate((c_ref, d_ref)):
            out_ref[g, 2 + i] = to_tiles(ref[g * 8 : (g + 1) * 8]).astype(BF)


def pack_states(ups, downs, groups):
    rows, cols = ups[0].shape
    return pl.pallas_call(
        pack_body,
        out_shape=jax.ShapeDtypeStruct((groups, 4, rows, cols // groups), BF),
        name="pack_states",
    )(*ups, *downs)


def order_body(old_ref, new_ref, in_ref, out_ref):
    copies = out_ref.shape[0] // in_ref.shape[0]
    for k in range(in_ref.shape[0]):
        for i in range(copies):
            out_ref[new_ref[k] * copies + i] = in_ref[old_ref[k]]


def order_states(old, new, shares, copies):
    shape = (shares.shape[0] * copies,) + shares.shape[1:]
    return pl.pallas_call(
        order_body, in_specs=[smem(), smem(), vmem()], out_shape=jax.ShapeDtypeStruct(shape, BF)
    )(old, new, shares)


def weight_grad_body(half_ref, a_ref, ao_ref, b_ref, bo_ref, out_ref):
    dims = (((0,), (0,)), ((), ()))
    total = lax.dot_general(a_ref[...], b_ref[...], dims, preferred_element_type=F32)
    total += lax.dot_general(ao_ref[...], bo_ref[...], dims, preferred_element_type=F32)
    out_ref[...] = total.astype(BF)


def weight_grad(place, a, a_other, b, b_other, step):
    rows, width = a.shape
    cols = b.shape[1]
    steps = width // 2 // step
    left = pl.BlockSpec(
        (rows, step), lambda i, at: (0, at[0] * steps + lax.rem(at[1] + i, steps))
    )
    right = pl.BlockSpec((rows, cols), lambda i, at: (0, 0))
    return pl.pallas_call(
        weight_grad_body,
        grid_spec=pltpu.PrefetchScalarGridSpec(
            num_scalar_prefetch=1,
            grid=(steps,),
            in_specs=[left, left, right, right],
            out_specs=pl.BlockSpec((step, cols), lambda i, at: (i, 0)),
        ),
        out_shape=jax.ShapeDtypeStruct((width // 2, cols), BF),
    )(place, a, a_other, b, b_other)


def flip_body(core_ref, own_ref, other_ref, out_ref):
    rows = own_ref.shape[0]
    out_ref[:, 0:rows] = own_ref[...].astype(F32).T.astype(BF)
    out_ref[:, rows : 2 * rows] = other_ref[...].astype(F32).T.astype(BF)


def flip(place, own, other, step=256):
    rows, width = own.shape
    steps = width // 2 // step
    part = pl.BlockSpec((rows, step), lambda i, at: (0, at[0] * steps + i))
    return pl.pallas_call(
        flip_body,
        grid_spec=pltpu.PrefetchScalarGridSpec(
            num_scalar_prefetch=1,
            grid=(steps,),
            in_specs=[part, part],
            out_specs=pl.BlockSpec((step, 2 * rows), lambda i, at: (i, 0)),
        ),
        out_shape=jax.ShapeDtypeStruct((width // 2, 2 * rows), BF),
        name="flip",
    )(place, own, other)


def up_grad_body(xt_ref, own_ref, other_ref, out_ref):
    rows = own_ref.shape[0]
    total = jnp.dot(xt_ref[:, 0:rows], own_ref[...], preferred_element_type=F32)
    total += jnp.dot(xt_ref[:, rows : 2 * rows], other_ref[...], preferred_element_type=F32)
    out_ref[...] = total.astype(BF)


def up_grad_part(flipped, own, other, steps=4):
    width, deep = flipped.shape
    rows, cols = own.shape
    right = pl.BlockSpec((rows, cols), lambda i: (0, 0))
    return pl.pallas_call(
        up_grad_body,
        grid=(steps,),
        in_specs=[pl.BlockSpec((width // steps, deep), lambda i: (i, 0)), right, right],
        out_specs=pl.BlockSpec((width // steps, cols), lambda i: (i, 0)),
        out_shape=jax.ShapeDtypeStruct((width, cols), BF),
        name="up_part",
    )(flipped, own, other)


def back_body(at_ref, dy_ref, slopes_ref, *refs):
    pieces, out_ref = refs[:-1], refs[-1]
    dims = (((1,), (1,)), ((), ()))
    per_core = len(pieces) // NC
    dy = dy_ref[...]
    for k in range(NC):
        own, above, low, high, below = (p[...] for p in pieces[k * per_core : (k + 1) * per_core])
        core = at_ref[0] if k == 0 else 1 - at_ref[0]
        for first, group in ((0, [own, above]), (2, [low, high, below])):
            both = lax.dot_general(
                dy, jnp.concatenate(group, axis=0), dims, preferred_element_type=F32
            )
            for i in range(2):
                tile = core * NY + lax.rem(at_ref[1] + first + i, NY)
                lanes = pl.ds(pl.multiple_of(tile * LANE, LANE), LANE)
                value = both[:, i * LANE : (i + 1) * LANE] * slopes_ref[:, lanes]
                out_ref[:, lanes] = value.astype(BF)


def back_grad(place, dy, slopes, pieces):
    return pl.pallas_call(
        back_body,
        in_specs=[smem(), vmem(), vmem()] + [vmem()] * len(pieces),
        out_shape=jax.ShapeDtypeStruct(slopes.shape, BF),
        name="back",
    )(place, dy, slopes, *pieces)


def relay_body(part_ref, below_ref, above_ref, up_ref, down_ref):
    tall = below_ref.shape[0]
    wide = 2 * tall
    mine = part_ref[wide : 2 * wide].astype(F32)
    up_ref[0:tall] = (mine[0:tall] + below_ref[...].astype(F32)).astype(BF)
    up_ref[tall:wide] = part_ref[wide + tall : 2 * wide]
    mine = part_ref[3 * wide + tall : 4 * wide].astype(F32)
    down_ref[0:tall] = part_ref[3 * wide : 3 * wide + tall]
    down_ref[tall:wide] = (mine + above_ref[...].astype(F32)).astype(BF)


def relay(part, below, above):
    tall, cols = below.shape
    out = jax.ShapeDtypeStruct((2 * tall, cols), BF)
    return pl.pallas_call(relay_body, out_shape=(out, out), name="relay")(part, below, above)


def finish_body(x_ref, part_ref, below_ref, above_ref, own_ref, send_ref):
    tall = own_ref.shape[0]
    total = part_ref[...].astype(F32) + below_ref[...].astype(F32) + above_ref[...].astype(F32)
    low, high = total[0:tall], total[tall : 2 * tall]
    first = x_ref[0] == 0
    own_ref[...] = jnp.where(first, low, high)
    send_ref[...] = jnp.where(first, high, low).astype(BF)


def finish(x_at, part, below, above):
    wide, cols = below.shape
    whole = pl.BlockSpec((wide, cols), lambda i: (0, 0))
    half_spec = pl.BlockSpec((wide // 2, cols), lambda i: (0, 0))
    return pl.pallas_call(
        finish_body,
        grid=(1,),
        in_specs=[smem(), whole, whole, whole],
        out_specs=(half_spec, half_spec),
        out_shape=(
            jax.ShapeDtypeStruct((wide // 2, cols), F32),
            jax.ShapeDtypeStruct((wide // 2, cols), BF),
        ),
        name="finish",
    )(x_at, part, below, above)


def adam_update(weight, moment, second, gradient):
    moment_new = beta_one * moment + (1.0 - beta_one) * gradient
    second_new = beta_two * second + (1.0 - beta_two) * gradient * gradient
    update = moment_new / bias_one / (jnp.sqrt(second_new / bias_two) + eps_value)
    return (weight - rate_value * (update + decay_value * weight), moment_new, second_new)


def adam_up_body(x_ref, weight_ref, state_ref, grad_ref, other_ref, *outs):
    rows = other_ref.shape[0]
    own = grad_ref[pl.ds(pl.multiple_of(x_ref[0] * rows, 16), rows)]
    both = own.astype(F32) + other_ref[...].astype(F32)
    grad = lanes_taken(both, inverse(row_order()))
    for g in range(state_ref.shape[0]):
        lanes = slice(g * LANE, (g + 1) * LANE)
        m, v = (state_ref[g, i].astype(F32) for i in range(2))
        w = weight_ref[g * NX + x_ref[0], 0].astype(F32)
        for ref, value in zip(outs, adam_update(w, m, v, grad[:, lanes])):
            ref[:, lanes] = value


def adam_down_body(x_ref, weight_ref, state_ref, grad_ref, other_ref, *outs):
    for g in range(state_ref.shape[0]):
        rows = slice(g * 8, (g + 1) * 8)
        m, v = (from_tiles(state_ref[g, i].astype(F32)) for i in range(2))
        w = from_tiles(weight_ref[g * NX + x_ref[0], 0].astype(F32))
        grad = grad_ref[rows] + other_ref[rows].astype(F32)
        for ref, value in zip(outs, adam_update(w, m, v, grad)):
            ref[rows] = value


def adam(body, x_at, weights, states, which, grads, shape):
    groups, _, rows, wide = states.shape
    full = pl.BlockSpec(shape, lambda i: (0, 0))
    return pl.pallas_call(
        body,
        grid=(1,),
        in_specs=[
            smem(),
            pl.BlockSpec((weights.shape[0], 1, rows, wide), lambda i: (0, which, 0, 0)),
            pl.BlockSpec((groups, 2, rows, wide), lambda i: (0, which, 0, 0)),
        ]
        + [pl.BlockSpec(g.shape, lambda i: (0, 0)) for g in grads],
        out_specs=[full] * 3,
        out_shape=[jax.ShapeDtypeStruct(shape, F32)] * 3,
    )(x_at, weights, states, *grads)


def silu_parts(pre_act):
    sigma = jax.nn.sigmoid(pre_act)
    return (pre_act * sigma, sigma * (1.0 + pre_act * (1.0 - sigma)))


def exchange(array, axis):
    return lax.all_to_all(array, axis, split_axis=0, concat_axis=0, tiled=True)


def from_partner(array):
    return lax.ppermute(array, "core", [(0, 1), (1, 0)])


def step(
    tokens,
    cotangent,
    block_expert,
    block_count,
    old_owner,
    new_owner,
    up_weight,
    down_weight,
    up_first,
    up_second,
    down_first,
    down_second,
):
    groups = lax.axis_size("expert")
    tok_rows, features = tokens.shape
    blocks = block_count.shape[0]
    rows = tok_rows // blocks
    core_at = lax.axis_index("core").astype(jnp.int32)
    y_at = lax.axis_index("y").astype(jnp.int32)
    x_at = lax.axis_index("x").astype(jnp.int32).reshape(1)
    down_place = jnp.stack([core_at, y_at])
    up_shape, down_shape = up_weight.shape[1:], down_weight.shape[1:]

    packed = pack_weights(up_weight[0], down_weight[0], groups)
    spread = exchange(packed, "expert")
    ordered = order_states(old_owner, new_owner, spread, NX)
    weights = exchange(ordered, ("expert", "x"))
    up_pair, down_pair = unpack_weights(weights, up_shape, down_shape)
    up_mat = lax.all_gather(up_pair, ("core", "y"), axis=0, tiled=True)
    rising = [(i, (i + 1) % NY) for i in range(NY)]
    falling = [(i, (i - 1) % NY) for i in range(NY)]
    tall = down_shape[0]
    w_below = lax.ppermute(down_pair, "y", rising)
    w_above = lax.ppermute(down_pair, "y", falling)
    w_low = lax.ppermute(w_below[:tall], "y", rising)
    w_high = lax.ppermute(w_above[tall:], "y", falling)
    pieces = (down_pair, w_above, w_low, w_high, w_below)
    pieces += tuple(from_partner(piece) for piece in pieces)

    send_x, send_dy = dispatch(
        block_expert,
        block_count,
        new_owner,
        tokens.reshape(blocks, rows, features),
        cotangent.reshape(blocks, rows, features),
    )
    send_x, _ = lax.optimization_barrier((send_x, down_pair))
    inputs = exchange(send_x, "expert")
    send_dy, inputs = lax.optimization_barrier((send_dy, inputs))
    inputs = inputs.reshape(-1, features)
    upstream = exchange(send_dy, "expert").reshape(-1, features)
    inputs_other, upstream_other = from_partner(inputs), from_partner(upstream)

    flipped = flip(down_place, inputs, inputs_other)

    packed = pack_states(
        (up_first[0], up_second[0]), (down_first[0], down_second[0]), groups
    )
    packed, upstream, flipped = lax.optimization_barrier((packed, upstream, flipped))
    shares = exchange(packed, "expert")

    pre_act = jnp.dot(inputs, up_mat, preferred_element_type=F32)
    active, slopes = silu_parts(pre_act)
    hidden = active.astype(BF)
    hidden_other = from_partner(hidden)
    pre_grad = back_grad(down_place, upstream, slopes, pieces)
    pre_grad_other = from_partner(pre_grad)
    up_part = up_grad_part(flipped, pre_grad, pre_grad_other)
    up_sum = lax.psum_scatter(up_part, "y", scatter_dimension=0, tiled=True)
    down_late, _ = lax.optimization_barrier((down_place, up_part))
    down_part = weight_grad(down_late, hidden, hidden_other, upstream, upstream_other, 128)
    below = lax.ppermute(down_part[4 * tall : 5 * tall], "y", rising)
    above = lax.ppermute(down_part[5 * tall : 6 * tall], "y", falling)
    ordered = order_states(old_owner, new_owner, shares, 1)
    ordered, pre_grad, _ = lax.optimization_barrier((ordered, pre_grad, down_part))
    states = exchange(ordered, "expert")
    input_grad = lax.dot_general(
        pre_grad, up_mat, (((1,), (1,)), ((), ())), preferred_element_type=F32
    ).astype(BF)
    down_part, input_grad = lax.optimization_barrier((down_part, input_grad))
    going_up, going_down = relay(down_part, below, above)
    below = lax.ppermute(going_up, "y", rising)
    above = lax.ppermute(going_down, "y", falling)
    input_grad, states = lax.optimization_barrier((input_grad, states))
    returned = exchange(input_grad.reshape(-1, rows, features), "expert")
    token_grad = combine(block_expert, new_owner, returned).reshape(tok_rows, features)

    swap = [(0, 1), (1, 0)]
    down_own, down_send = finish(x_at, down_part, below, above)
    down_other = lax.ppermute(down_send, "x", swap)
    up_send = lax.dynamic_slice_in_dim(up_sum, (1 - x_at[0]) * up_shape[0], up_shape[0])
    up_other = lax.ppermute(up_send, "x", swap)
    down_new = adam(adam_down_body, x_at, weights, states, 1, (down_own, down_other), down_shape)
    up_new = adam(adam_up_body, x_at, weights, states, 0, (up_sum, up_other), up_shape)
    return (
        token_grad,
        up_new[0][None],
        down_new[0][None],
        up_new[1][None],
        up_new[2][None],
        down_new[1][None],
        down_new[2][None],
    )


def solution(mesh):
    fine = Mesh(
        mesh.devices.reshape(mesh.devices.shape[0], NX, NY, NC), ("expert", "x", "y", "core")
    )
    every = ("expert", "x", "y", "core")
    dp = ("x", "y", "core")
    state = P("expert", dp, None)
    return jax.shard_map(
        step,
        mesh=fine,
        in_specs=(P(every, None), P(every, None), P(every, None), P(every), P(), P())
        + (state,) * 6,
        out_specs=(P(every, None),) + (state,) * 6,
        check_vma=False,
    )
```
